256 devices in a mesh: rows: 64 (over x, z, y_hi), cols: 4 (over y_lo, core).
Axes of the slice: x: 4, y: 4 (y_hi: 2, y_lo: 2; y = y_hi * 2 + y_lo), z: 8, core: 2. Of those that a mesh axis runs over, the one named last changes fastest.
Arguments:
- matrix: float32 [4096, 32, 2, 128], P('rows', 'cols'), may hold values from -54 to 54
- plan: int32 [2, 4, 256], replicated, may hold values from 0 to 255, as said below
Outputs:
- rotated: float32 [4096, 32, 2, 128], P('rows', 'cols')
The draws below stay inside these ranges and needn't reach their ends.
Inputs may be any that keep to these rules, and one draw needn't show every extreme that they name: Each plan[s, r] pairs the 256 columns: partner of partner of i is i, and no column is its own partner.
All inputs are finite; a program needn't handle non-finite values.
Results may differ from the reference program's by a relative error of at most 0.0003.
Values sent between devices are 32-bit elements; how exact they have to be, the bound alone decides.
A program may use at most 128 MiB of HBM per device.

```python
import math
import jax
import jax.numpy as jnp
from jax import lax

BLOCK = 128
PAIR_DEV = 8
STEPS = 2
ROUNDS = 4
PAIRS = 32
ROWS = 4096


def draw_matrix(key, part):
    base_key = jax.random.fold_in(key, 11)
    first, second, third = jax.random.split(base_key, 3)
    shape = (ROWS, PAIRS, 2, BLOCK)
    row_scale = jnp.exp(jax.random.uniform(second, (ROWS, 1, 1, 1), jnp.float32, math.log(0.3), math.log(3.0)))
    col_scale = jnp.exp(jax.random.uniform(third, (1, PAIRS, 2, BLOCK), jnp.float32, math.log(0.3), math.log(3.0)))
    values = jnp.clip(jax.random.normal(first, shape, jnp.float32), -6.0, 6.0)
    return (values * row_scale * col_scale).astype(jnp.float32)


def draw_plan(key, part):
    width = 2 * BLOCK

    def one_table(inner_key):
        order = jax.random.permutation(inner_key, width).astype(jnp.int32)
        first_half = order[0::2]
        second_half = order[1::2]
        partner = jnp.zeros((width,), jnp.int32).at[first_half].set(second_half).at[second_half].set(first_half)
        return partner
    keys = jax.random.split(jax.random.fold_in(key, 7), STEPS * ROUNDS)
    tables = jax.vmap(one_table)(keys)
    return tables.reshape(STEPS, ROUNDS, width).astype(jnp.int32)


def setup_inputs(seed: int = 0) -> dict:
    streams_of = jax.random.split(jax.random.key(seed), 3)
    return {
        "matrix": draw_matrix(jax.random.fold_in(streams_of[2], 71), 0),
        "plan": draw_plan(jax.random.fold_in(streams_of[2], 71), 0),
    }


def diagonalize(grams, table):
    width = grams.shape[1]
    indices = jnp.arange(width, dtype=jnp.int32)
    rotation = jnp.broadcast_to(jnp.eye(width, dtype=jnp.float32), grams.shape)
    unit_matrix = jnp.eye(width, dtype=jnp.float32)
    for round_index in range(table.shape[0]):
        partner = table[round_index]
        onehot = (partner[:, None] == indices[None, :]).astype(jnp.float32)
        diagonal_now = jnp.diagonal(grams, axis1=1, axis2=2)
        partner_diag = jnp.einsum('pj,ij->pi', diagonal_now, onehot, precision=lax.Precision.HIGHEST)
        partner_gram = lax.optimization_barrier(jnp.sum(grams * onehot[None], axis=2))
        orient = jnp.where(indices < partner, 1.0, -1.0).astype(jnp.float32)
        spread = orient[None, :] * (partner_diag - diagonal_now)
        sign_part = jnp.where(spread >= 0.0, 1.0, -1.0).astype(jnp.float32)
        tangent = sign_part * 2.0 * partner_gram / (jnp.abs(spread) + jnp.sqrt(spread * spread + 4.0 * partner_gram * partner_gram))
        cosine = 1.0 / jnp.sqrt(1.0 + tangent * tangent)
        sine_part = tangent * cosine
        off_part = jnp.swapaxes(onehot[None] * (-orient[None, :] * sine_part)[:, :, None], 1, 2)
        rot_now = cosine[:, :, None] * unit_matrix[None] + off_part
        product = jnp.einsum('pij,pjk->pik', grams, rot_now, precision=lax.Precision.HIGHEST)
        grams = jnp.einsum('pji,pjk->pik', rot_now, product, precision=lax.Precision.HIGHEST)
        rotation = jnp.einsum('pij,pjk->pik', rotation, rot_now, precision=lax.Precision.HIGHEST)
    return (grams, rotation)

def reference(matrix, plan):
    rows_all, pairs, halves, width = matrix.shape
    columns = matrix.reshape(rows_all, pairs, halves * width)
    for step_index in range(STEPS):
        grams = jnp.einsum('mpi,mpj->pij', columns, columns, precision=lax.Precision.HIGHEST)
        grams, rotation = diagonalize(grams, plan[step_index])
        columns = jnp.einsum('mpi,pij->mpj', columns, rotation, precision=lax.Precision.HIGHEST)
        quarter = columns.reshape(rows_all, pairs, halves, width)
        tops = quarter[:, :, 0, :]
        bottoms = jnp.roll(quarter[:, :, 1, :], PAIR_DEV, axis=1)
        columns = jnp.stack([tops, bottoms], axis=2).reshape(rows_all, pairs, halves * width)
    return columns.reshape(matrix.shape)
```

```python
import functools

import jax
import jax.numpy as jnp
from jax import lax
from jax.experimental import pallas as pl
from jax.experimental.pallas import tpu as pltpu
from jax.sharding import PartitionSpec as P

MESH = pl.DeviceIdType.MESH
XS, ZS, YS, CS = 4, 8, 2, 4
GROUP = XS * YS
BLOCK = 128
WIDTH = 2 * BLOCK
PEERS = ((2, 1), (1, 1), (3, 1), (2, 0), (0, 1), (1, 0), (3, 0))
RING = (4, 3, 5, 2, 6, 1, 7)
FIRST = (((0,), (0,)), ((), ()))
PLAIN = (((1,), (0,)), ((), ()))


def parts_of(value):
    high = value.astype(jnp.bfloat16)
    rest = value - high.astype(jnp.float32)
    middle = rest.astype(jnp.bfloat16)
    low = (rest - middle.astype(jnp.float32)).astype(jnp.bfloat16)
    return high, middle, low


def product(a, b, dims):
    return lax.dot_general(a, b, dims, preferred_element_type=jnp.float32)


def full_product(a, b, dims=PLAIN):
    return lax.dot_general(
        a, b, dims, precision=lax.Precision.HIGHEST, preferred_element_type=jnp.float32
    )


def times_onehot(parts, onehot):
    high, middle, low = parts
    return product(high, onehot, PLAIN) + (product(middle, onehot, PLAIN) + product(low, onehot, PLAIN))


def onehot_times(onehot, parts):
    high, middle, low = parts
    return product(onehot, high, PLAIN) + (product(onehot, middle, PLAIN) + product(onehot, low, PLAIN))


def solve(gram, plan_of_round, rounds, final_gram):
    below = lax.broadcasted_iota(jnp.int32, (WIDTH, WIDTH), 0)
    along = lax.broadcasted_iota(jnp.int32, (WIDTH, WIDTH), 1)
    unit = below == along
    index = lax.broadcasted_iota(jnp.int32, (1, WIDTH), 1)
    rotation = None
    for r in range(rounds):
        partner = plan_of_round(r)
        pairing = below == partner
        onehot = pairing.astype(jnp.float32).astype(jnp.bfloat16)
        moved = times_onehot(parts_of(gram), onehot)
        own = jnp.sum(jnp.where(unit, gram, 0.0), axis=0, keepdims=True)
        cross = jnp.sum(jnp.where(pairing, gram, 0.0), axis=0, keepdims=True)
        other = jnp.sum(jnp.where(pairing, moved, 0.0), axis=0, keepdims=True)
        orient = jnp.where(index < partner, 1.0, -1.0)
        spread = orient * (other - own)
        sign = jnp.where(spread >= 0.0, 1.0, -1.0)
        tangent = sign * 2.0 * cross / (jnp.abs(spread) + jnp.sqrt(spread * spread + 4.0 * cross * cross))
        cosine = 1.0 / jnp.sqrt(1.0 + tangent * tangent)
        sine = -orient * (tangent * cosine)
        if r + 1 < rounds or final_gram:
            both = onehot_times(onehot, parts_of(moved))
            cosine_down = jnp.transpose(jnp.broadcast_to(cosine, (BLOCK, WIDTH)))
            sine_down = jnp.transpose(jnp.broadcast_to(sine, (BLOCK, WIDTH)))
            cosine_down = jnp.concatenate([cosine_down, cosine_down], axis=1)
            sine_down = jnp.concatenate([sine_down, sine_down], axis=1)
            gram = (cosine_down * cosine * gram + sine_down * sine * both) + (
                cosine_down * sine * moved + sine_down * cosine * jnp.transpose(moved)
            )
        if rotation is None:
            rotation = jnp.where(unit, cosine, 0.0) + jnp.where(pairing, sine, 0.0)
        else:
            rotation = rotation * cosine + times_onehot(parts_of(rotation), onehot) * sine
    return gram, rotation


def kernel(
    x_hbm,
    plan_hbm,
    out_hbm,
    plan_ref,
    x_own,
    tops,
    bottoms,
    partial,
    shares_tt,
    shares_b,
    total,
    total_mine,
    bottoms_out,
    bottoms_in,
    square_out,
    square_in,
    tops_now,
    partial_tb,
    shares_tb,
    total_tb,
    total_tb_mine,
    result_out,
    result_in,
    load_sem,
    in_send,
    in_recv,
    sum_send,
    sum_recv,
    all_send,
    all_recv,
    next_send,
    next_recv,
    sum2_send,
    sum2_recv,
    all2_send,
    all2_recv,
    out_send,
    out_recv,
    store_sem,
):
    rows = lax.axis_index("rows")
    col = lax.axis_index("cols")
    x = rows // (ZS * YS)
    z = (rows // YS) % ZS
    y = rows % YS
    me = x * YS + y
    chunk = x_own.shape[1]
    every = tops.shape[0]
    share = BLOCK // ZS

    def member(a, b):
        return ((x + a) % XS) * YS + (y + b) % YS

    def source(a, b):
        return ((x + XS - a) % XS) * YS + (y + YS - b) % YS

    def row_of(a, b):
        return (((x + a) % XS) * ZS + z) * YS + (y + b) % YS

    def ring_row(d):
        return (x * ZS + (z + d) % ZS) * YS + y

    after = (col + 1) % CS
    before = (col + CS - 1) % CS

    barrier = pltpu.get_barrier_semaphore()

    def greet(row, column):
        pl.semaphore_signal(barrier, inc=1, device_id=(row, column), device_id_type=MESH)

    for a, b in PEERS:
        greet(row_of(a, b), col)
        greet(row_of(a, b), before)
    greet(rows, before)
    for d in RING:
        greet(ring_row(d), col)

    def remote(src, dst, send, recv, row, column):
        return pltpu.make_async_remote_copy(
            src_ref=src, dst_ref=dst, send_sem=send, recv_sem=recv, device_id=(row, column), device_id_type=MESH
        )

    plan_copy = pltpu.make_async_copy(plan_hbm, plan_ref, load_sem.at[8, 0])
    own_place = pl.ds(pl.multiple_of(me * chunk, chunk), chunk)
    loads = {}
    for half in range(2):
        for k, (a, b) in enumerate(PEERS):
            slot = 2 * member(a, b) + half
            loads[k, half] = pltpu.make_async_copy(x_hbm.at[:, slot, :], x_own.at[slot], load_sem.at[k, half])
        gathered = (tops, bottoms)[half]
        loads[7, half] = pltpu.make_async_copy(x_hbm.at[:, 2 * me + half, :], gathered.at[own_place], load_sem.at[7, half])
    for half in range(2):
        for k in range(8):
            loads[k, half].start()
    plan_copy.start()

    pl.semaphore_wait(barrier, 2 * len(PEERS) + 1 + len(RING))

    incoming = {}
    for half in range(2):
        gathered = (tops, bottoms)[half]
        for k, (a, b) in enumerate(PEERS):
            loads[k, half].wait()
            incoming[k, half] = remote(
                x_own.at[2 * member(a, b) + half],
                gathered.at[own_place],
                in_send.at[k, half],
                in_recv.at[k, half],
                row_of(a, b),
                col,
            )
            incoming[k, half].start()
    plan_copy.wait()
    loads[7, 0].wait()
    loads[7, 1].wait()

    def ring_place(d):
        return pl.ds(pl.multiple_of(((z + d) % ZS) * share, share), share)

    for k in range(len(PEERS)):
        incoming[k, 0].wait_recv()
    top_now = tops[...]
    partial[0] = full_product(top_now, top_now, FIRST)
    sums = {}
    for n, d in enumerate(RING):
        sums[n, 0] = remote(
            partial.at[0, ring_place(d)], shares_tt.at[n], sum_send.at[n, 0], sum_recv.at[n, 0], ring_row(d), col
        )
        sums[n, 0].start()

    for k in range(len(PEERS)):
        incoming[k, 1].wait_recv()
    bottom_now = bottoms[...]
    partial[1] = full_product(top_now, bottom_now, FIRST)
    partial[2] = full_product(bottom_now, bottom_now, FIRST)
    for n, d in enumerate(RING):
        sums[n, 1] = remote(
            partial.at[1:3, ring_place(d)], shares_b.at[n], sum_send.at[n, 1], sum_recv.at[n, 1], ring_row(d), col
        )
        sums[n, 1].start()

    spread = {}
    here = ring_place(0)
    for n in range(len(RING)):
        sums[n, 0].wait_recv()
    mine = partial[0, here]
    for n in range(len(RING)):
        mine = mine + shares_tt[n]
    total_mine[0] = mine
    total[0, here] = mine
    for n, d in enumerate(RING):
        spread[n, 0] = remote(
            total_mine.at[0], total.at[0, here], all_send.at[n, 0], all_recv.at[n, 0], ring_row(d), col
        )
        spread[n, 0].start()
    for n in range(len(RING)):
        sums[n, 1].wait_recv()
    mine = partial[1:3, here]
    for n in range(len(RING)):
        mine = mine + shares_b[n]
    total_mine[1:3] = mine
    total[1:3, here] = mine
    for n, d in enumerate(RING):
        spread[n, 1] = remote(
            total_mine.at[1:3], total.at[1:3, here], all_send.at[n, 1], all_recv.at[n, 1], ring_row(d), col
        )
        spread[n, 1].start()
    for n in range(len(RING)):
        spread[n, 0].wait_recv()
        spread[n, 1].wait_recv()

    cross = total[1]
    gram = jnp.concatenate(
        [jnp.concatenate([total[0], cross], axis=1), jnp.concatenate([jnp.transpose(cross), total[2]], axis=1)], axis=0
    )
    rounds = plan_ref.shape[1]
    gram, rotation = solve(gram, lambda r: plan_ref[0, r : r + 1, :], rounds, True)
    top_square = gram[:BLOCK, :BLOCK]
    square_out[...] = gram[BLOCK:, BLOCK:]
    square = remote(square_out, square_in, next_send.at[0], next_recv.at[0], rows, after)
    square.start()
    pieces = 4
    piece = every // pieces
    moves = []
    for n in range(pieces):
        place = pl.ds(n * piece, piece)
        now = full_product(jnp.concatenate([tops[place], bottoms[place]], axis=1), rotation)
        tops_now[place] = now[:, :BLOCK]
        bottoms_out[place] = now[:, BLOCK:]
        move = remote(
            bottoms_out.at[place], bottoms_in.at[place], next_send.at[1 + n], next_recv.at[1 + n], rows, after
        )
        move.start()
        moves.append(move)

    square.wait_recv()
    cross = jnp.zeros((BLOCK, BLOCK), jnp.float32)
    for n in range(pieces):
        place = pl.ds(n * piece, piece)
        moves[n].wait_recv()
        cross = cross + full_product(tops_now[place], bottoms_in[place], FIRST)
    partial_tb[...] = cross
    sums2 = []
    for n, d in enumerate(RING):
        copy = remote(partial_tb.at[ring_place(d)], shares_tb.at[n], sum2_send.at[n], sum2_recv.at[n], ring_row(d), col)
        copy.start()
        sums2.append(copy)
    for copy in sums2:
        copy.wait_recv()
    mine = partial_tb[here]
    for n in range(len(RING)):
        mine = mine + shares_tb[n]
    total_tb_mine[...] = mine
    total_tb[here] = mine
    spread2 = []
    for n, d in enumerate(RING):
        copy = remote(total_tb_mine, total_tb.at[here], all2_send.at[n], all2_recv.at[n], ring_row(d), col)
        copy.start()
        spread2.append(copy)
    for copy in spread2:
        copy.wait_recv()
    cross = total_tb[...]
    gram = jnp.concatenate(
        [jnp.concatenate([top_square, cross], axis=1), jnp.concatenate([jnp.transpose(cross), square_in[...]], axis=1)],
        axis=0,
    )
    _, rotation = solve(gram, lambda r: plan_ref[1, r : r + 1, :], rounds, False)

    outgoing = {}
    stores = []
    for k, (a, b) in enumerate(PEERS + ((0, 0),)):
        target = member(a, b)
        place = pl.ds(pl.multiple_of(target * chunk, chunk), chunk)
        now = full_product(jnp.concatenate([tops_now[place], bottoms_in[place]], axis=1), rotation)
        result_out[k, 0] = now[:, :BLOCK]
        result_out[k, 1] = now[:, BLOCK:]
        outgoing[k, 1] = remote(
            result_out.at[k, 1], result_in.at[2 * me + 1], out_send.at[k, 1], out_recv.at[k, 1], row_of(a, b), after
        )
        outgoing[k, 1].start()
        if k < len(PEERS):
            outgoing[k, 0] = remote(
                result_out.at[k, 0], result_in.at[2 * me], out_send.at[k, 0], out_recv.at[k, 0], row_of(a, b), col
            )
            outgoing[k, 0].start()
        else:
            store = pltpu.make_async_copy(result_out.at[k, 0], out_hbm.at[:, 2 * me, :], store_sem.at[k, 0])
            store.start()
            stores.append(store)
    for k, (a, b) in enumerate(PEERS + ((0, 0),)):
        for half in (1, 0):
            if (k, half) not in outgoing:
                continue
            outgoing[k, half].wait_recv()
            slot = 2 * source(a, b) + half
            store = pltpu.make_async_copy(result_in.at[slot], out_hbm.at[:, slot, :], store_sem.at[k, half])
            store.start()
            stores.append(store)

    for copies in (incoming, sums, spread, outgoing):
        for copy in copies.values():
            copy.wait_send()
    for copy in [square, *moves, *sums2, *spread2]:
        copy.wait_send()
    for store in stores:
        store.wait()


def body(matrix, plan):
    chunk, pairs, halves, width = matrix.shape
    slots = pairs * halves
    every = chunk * GROUP
    share = BLOCK // ZS
    f32 = jnp.float32
    dma = pltpu.SemaphoreType.DMA
    near, ring = len(PEERS), len(RING)
    vmem = pltpu.VMEM
    result = pl.pallas_call(
        kernel,
        out_shape=jax.ShapeDtypeStruct((chunk, slots, width), f32),
        in_specs=[pl.BlockSpec(memory_space=pl.ANY)] * 2,
        out_specs=pl.BlockSpec(memory_space=pl.ANY),
        scratch_shapes=[
            vmem(plan.shape, jnp.int32),
            vmem((slots, chunk, width), f32),
            vmem((every, width), f32),
            vmem((every, width), f32),
            vmem((3, BLOCK, BLOCK), f32),
            vmem((ring, share, BLOCK), f32),
            vmem((ring, 2, share, BLOCK), f32),
            vmem((3, BLOCK, BLOCK), f32),
            vmem((3, share, BLOCK), f32),
            vmem((every, width), f32),
            vmem((every, width), f32),
            vmem((BLOCK, BLOCK), f32),
            vmem((BLOCK, BLOCK), f32),
            vmem((every, width), f32),
            vmem((BLOCK, BLOCK), f32),
            vmem((ring, share, BLOCK), f32),
            vmem((BLOCK, BLOCK), f32),
            vmem((share, BLOCK), f32),
            vmem((near + 1, 2, chunk, width), f32),
            vmem((slots, chunk, width), f32),
            dma((9, 2)),
            dma((near, 2)),
            dma((near, 2)),
            dma((ring, 2)),
            dma((ring, 2)),
            dma((ring, 2)),
            dma((ring, 2)),
            dma((5,)),
            dma((5,)),
            dma((ring,)),
            dma((ring,)),
            dma((ring,)),
            dma((ring,)),
            dma((near + 1, 2)),
            dma((near + 1, 2)),
            dma((near + 1, 2)),
        ],
        compiler_params=pltpu.CompilerParams(collective_id=0, has_side_effects=True),
        cost_estimate=pl.CostEstimate(flops=10**9, bytes_accessed=2 * matrix.size * 4, transcendentals=0),
        name="jacobi_steps",
    )(matrix.reshape(chunk, slots, width), plan)
    return result.reshape(matrix.shape)


def solution(mesh):
    in_specs = (P("rows", "cols", None, None), P())
    out_specs = P("rows", "cols", None, None)
    return jax.shard_map(body, mesh=mesh, in_specs=in_specs, out_specs=out_specs, check_vma=False)
```

```python
import functools

import jax
import jax.numpy as jnp
from jax import lax
from jax.experimental import pallas as pl
from jax.experimental.pallas import tpu as pltpu
from jax.sharding import PartitionSpec as P

MESH = pl.DeviceIdType.MESH
XS, ZS, YS, CS = 4, 8, 2, 4
GROUP = XS * YS
BLOCK = 128
WIDTH = 2 * BLOCK
PEERS = ((2, 1), (1, 1), (3, 1), (2, 0), (0, 1), (1, 0), (3, 0))
RING = (4, 3, 5, 2, 6, 1, 7)
FIRST = (((0,), (0,)), ((), ()))
PLAIN = (((1,), (0,)), ((), ()))


def parts_of(value):
    high = value.astype(jnp.bfloat16)
    rest = value - high.astype(jnp.float32)
    middle = rest.astype(jnp.bfloat16)
    low = (rest - middle.astype(jnp.float32)).astype(jnp.bfloat16)
    return high, middle, low


def product(a, b, dims):
    return lax.dot_general(a, b, dims, preferred_element_type=jnp.float32)


def full_product(a, b, dims=PLAIN):
    return lax.dot_general(
        a, b, dims, precision=lax.Precision.HIGHEST, preferred_element_type=jnp.float32
    )


def product_of(a, b, dims=PLAIN):
    high = product(a[0], b[0], dims)
    return high + (product(a[0], b[1], dims) + product(a[1], b[0], dims))


def columns_moved(value, partner):
    rows = value.shape[0]
    near = jnp.where(partner < BLOCK, partner, partner - BLOCK)
    sides = []
    for half in range(2):
        lanes = slice(half * BLOCK, (half + 1) * BLOCK)
        index = jnp.broadcast_to(near[:, lanes], (rows, BLOCK))
        left = jnp.broadcast_to(partner[:, lanes] < BLOCK, (rows, BLOCK))
        picked = [
            jnp.take_along_axis(value[:, n * BLOCK : (n + 1) * BLOCK], index, axis=1, mode="promise_in_bounds")
            for n in range(2)
        ]
        sides.append(jnp.where(left, picked[0], picked[1]))
    return jnp.concatenate(sides, axis=1)


def solve(gram, plan_of_round, rounds, final_gram):
    below = lax.broadcasted_iota(jnp.int32, (WIDTH, WIDTH), 0)
    along = lax.broadcasted_iota(jnp.int32, (WIDTH, WIDTH), 1)
    unit = below == along
    block_unit = unit[:BLOCK, :BLOCK]
    index = lax.broadcasted_iota(jnp.int32, (1, WIDTH), 1)
    rotation = None
    for r in range(rounds):
        partner = plan_of_round(r)
        pairing = below == partner
        moved = columns_moved(gram, partner)
        own = jnp.concatenate(
            [
                jnp.sum(jnp.where(block_unit, gram[:BLOCK, :BLOCK], 0.0), axis=0, keepdims=True),
                jnp.sum(jnp.where(block_unit, gram[BLOCK:, BLOCK:], 0.0), axis=0, keepdims=True),
            ],
            axis=1,
        )
        cross = jnp.sum(jnp.where(pairing, gram, 0.0), axis=0, keepdims=True)
        other = columns_moved(jnp.broadcast_to(own, (8, WIDTH)), partner)[:1]
        orient = jnp.where(index < partner, 1.0, -1.0)
        spread = orient * (other - own)
        sign = jnp.where(spread >= 0.0, 1.0, -1.0)
        tangent = sign * 2.0 * cross / (jnp.abs(spread) + jnp.sqrt(spread * spread + 4.0 * cross * cross))
        cosine = 1.0 / jnp.sqrt(1.0 + tangent * tangent)
        sine = -orient * (tangent * cosine)
        if r + 1 < rounds or final_gram:
            turned = jnp.transpose(gram * cosine + moved * sine)
            gram = turned * cosine + columns_moved(turned, partner) * sine
        if rotation is None:
            rotation = jnp.where(unit, cosine, 0.0) + jnp.where(pairing, sine, 0.0)
        else:
            rotation = rotation * cosine + columns_moved(rotation, partner) * sine
    return gram, rotation


def kernel(
    x_hbm,
    plan_hbm,
    result,
    plan_ref,
    x_own,
    tops,
    bottoms,
    partial,
    shares_tt,
    shares_b,
    total,
    total_mine,
    bottoms_out,
    bottoms_in,
    square_out,
    square_in,
    tops_now,
    partial_tb,
    shares_tb,
    total_tb,
    total_tb_mine,
    result_out,
    load_sem,
    in_send,
    in_recv,
    sum_send,
    sum_recv,
    all_send,
    all_recv,
    next_send,
    next_recv,
    sum2_send,
    sum2_recv,
    all2_send,
    all2_recv,
    out_send,
    out_recv,
):
    rows = lax.axis_index("rows")
    col = lax.axis_index("cols")
    x = rows // (ZS * YS)
    z = (rows // YS) % ZS
    y = rows % YS
    me = x * YS + y
    chunk = x_own.shape[1]
    every = tops.shape[0]
    share = BLOCK // ZS
    near, ring = len(PEERS), len(RING)

    def member(a, b):
        return ((x + a) % XS) * YS + (y + b) % YS

    def row_of(a, b):
        return (((x + a) % XS) * ZS + z) * YS + (y + b) % YS

    def ring_row(d):
        return (x * ZS + (z + d) % ZS) * YS + y

    after = (col + 1) % CS
    before = (col + CS - 1) % CS

    def send(src, dst, send_sem, recv_sem, row, column):
        pltpu.make_async_remote_copy(
            src_ref=src, dst_ref=dst, send_sem=send_sem, recv_sem=recv_sem, device_id=(row, column), device_id_type=MESH
        ).start()

    def await_bytes(like, sem):
        pltpu.make_async_remote_copy(
            src_ref=like, dst_ref=like, send_sem=sem, recv_sem=sem, device_id=(rows, col), device_id_type=MESH
        ).wait_recv()

    barrier = pltpu.get_barrier_semaphore()

    def greet(row, column):
        pl.semaphore_signal(barrier, inc=1, device_id=(row, column), device_id_type=MESH)

    for a, b in PEERS:
        greet(row_of(a, b), col)
        greet(row_of(a, b), before)
    greet(rows, before)
    for d in RING:
        greet(ring_row(d), col)

    own_place = pl.ds(pl.multiple_of(me * chunk, chunk), chunk)
    loads = ([], [])
    for half in range(2):
        for a, b in PEERS:
            slot = 2 * member(a, b) + half
            loads[half].append(pltpu.make_async_copy(x_hbm.at[:, slot, :], x_own.at[slot], load_sem.at[half]))
        gathered = (tops, bottoms)[half]
        loads[half].append(pltpu.make_async_copy(x_hbm.at[:, 2 * me + half, :], gathered.at[own_place], load_sem.at[half]))
        for load in loads[half]:
            load.start()
    plan_copy = pltpu.make_async_copy(plan_hbm, plan_ref, load_sem.at[2])
    plan_copy.start()

    pl.semaphore_wait(barrier, 2 * near + 1 + ring)

    for half in range(2):
        gathered = (tops, bottoms)[half]
        for load in loads[half]:
            load.wait()
        for a, b in PEERS:
            send(
                x_own.at[2 * member(a, b) + half],
                gathered.at[own_place],
                in_send,
                in_recv.at[half],
                row_of(a, b),
                col,
            )
    plan_copy.wait()

    def ring_place(d):
        return pl.ds(pl.multiple_of(((z + d) % ZS) * share, share), share)

    await_bytes(tops.at[: near * chunk], in_recv.at[0])
    top_now = tops[...]
    partial[0] = full_product(top_now, top_now, FIRST)
    for n, d in enumerate(RING):
        send(partial.at[0, ring_place(d)], shares_tt.at[n], sum_send, sum_recv.at[0], ring_row(d), col)

    await_bytes(bottoms.at[: near * chunk], in_recv.at[1])
    bottom_now = bottoms[...]
    partial[1] = full_product(top_now, bottom_now, FIRST)
    partial[2] = full_product(bottom_now, bottom_now, FIRST)
    for n, d in enumerate(RING):
        send(partial.at[1:3, ring_place(d)], shares_b.at[n], sum_send, sum_recv.at[1], ring_row(d), col)

    here = ring_place(0)
    await_bytes(shares_tt, sum_recv.at[0])
    mine = partial[0, here]
    for n in range(ring):
        mine = mine + shares_tt[n]
    total_mine[0] = mine
    total[0, here] = mine
    for d in RING:
        send(total_mine.at[0], total.at[0, here], all_send, all_recv.at[0], ring_row(d), col)
    await_bytes(shares_b, sum_recv.at[1])
    mine = partial[1:3, here]
    for n in range(ring):
        mine = mine + shares_b[n]
    total_mine[1:3] = mine
    total[1:3, here] = mine
    for d in RING:
        send(total_mine.at[1:3], total.at[1:3, here], all_send, all_recv.at[1], ring_row(d), col)
    await_bytes(total.at[0, : ring * share], all_recv.at[0])
    await_bytes(total.at[1:3, : ring * share], all_recv.at[1])

    cross = total[1]
    gram = jnp.concatenate(
        [jnp.concatenate([total[0], cross], axis=1), jnp.concatenate([jnp.transpose(cross), total[2]], axis=1)], axis=0
    )
    rounds = plan_ref.shape[1]
    gram, rotation = solve(gram, lambda r: plan_ref[0, r : r + 1, :], rounds, True)
    top_square = gram[:BLOCK, :BLOCK]
    square_out[...] = gram[BLOCK:, BLOCK:]
    send(square_out, square_in, next_send, next_recv.at[0], rows, after)
    pieces = 4
    piece = every // pieces
    columns = parts_of(jnp.concatenate([tops[...], bottoms[...]], axis=1))
    turn = parts_of(rotation)
    for n in range(pieces):
        place = pl.ds(n * piece, piece)
        lines = slice(n * piece, (n + 1) * piece)
        bottoms_out[place] = product_of([part[lines] for part in columns], [part[:, BLOCK:] for part in turn])
        send(bottoms_out.at[place], bottoms_in.at[place], next_send, next_recv.at[1 + n], rows, after)
    tops_now[...] = product_of(columns, [part[:, :BLOCK] for part in turn])

    await_bytes(square_in, next_recv.at[0])
    cross = jnp.zeros((BLOCK, BLOCK), jnp.float32)
    for n in range(pieces):
        place = pl.ds(n * piece, piece)
        await_bytes(bottoms_in.at[place], next_recv.at[1 + n])
        cross = cross + product_of(parts_of(tops_now[place]), parts_of(bottoms_in[place]), FIRST)
    partial_tb[...] = cross
    for n, d in enumerate(RING):
        send(partial_tb.at[ring_place(d)], shares_tb.at[n], sum2_send, sum2_recv, ring_row(d), col)
    await_bytes(shares_tb, sum2_recv)
    mine = partial_tb[here]
    for n in range(ring):
        mine = mine + shares_tb[n]
    total_tb_mine[...] = mine
    total_tb[here] = mine
    for d in RING:
        send(total_tb_mine, total_tb.at[here], all2_send, all2_recv, ring_row(d), col)
    await_bytes(total_tb.at[: ring * share], all2_recv)
    cross = total_tb[...]
    gram = jnp.concatenate(
        [jnp.concatenate([top_square, cross], axis=1), jnp.concatenate([jnp.transpose(cross), square_in[...]], axis=1)],
        axis=0,
    )
    _, rotation = solve(gram, lambda r: plan_ref[1, r : r + 1, :], rounds, False)

    turn = parts_of(rotation)
    for k, (a, b) in enumerate(PEERS + ((0, 0),)):
        place = pl.ds(pl.multiple_of(member(a, b) * chunk, chunk), chunk)
        now = product_of(parts_of(jnp.concatenate([tops_now[place], bottoms_in[place]], axis=1)), turn)
        result_out[k, 1] = now[:, BLOCK:]
        send(result_out.at[k, 1], result.at[2 * me + 1], out_send, out_recv, row_of(a, b), after)
        if k < near:
            result_out[k, 0] = now[:, :BLOCK]
            send(result_out.at[k, 0], result.at[2 * me], out_send, out_recv, row_of(a, b), col)
        else:
            result[2 * me] = now[:, :BLOCK]
    await_bytes(result.at[: 2 * near + 1], out_recv)
    await_bytes(x_own.at[: 2 * near], in_send)
    await_bytes(tops.at[: 3 * ring * share], sum_send)
    await_bytes(tops.at[: 3 * ring * share], all_send)
    await_bytes(tops, next_send)
    await_bytes(square_out, next_send)
    await_bytes(shares_tb, sum2_send)
    await_bytes(shares_tb, all2_send)
    await_bytes(result.at[: 2 * near + 1], out_send)


def body(matrix, plan):
    chunk, pairs, halves, width = matrix.shape
    slots = pairs * halves
    every = chunk * GROUP
    share = BLOCK // ZS
    f32 = jnp.float32
    dma = pltpu.SemaphoreType.DMA
    near, ring = len(PEERS), len(RING)
    vmem = pltpu.VMEM
    result = pl.pallas_call(
        kernel,
        out_shape=jax.ShapeDtypeStruct((slots, chunk, width), f32),
        in_specs=[pl.BlockSpec(memory_space=pltpu.HBM)] * 2,
        out_specs=pl.BlockSpec(memory_space=pltpu.VMEM),
        scratch_shapes=[
            vmem(plan.shape, jnp.int32),
            vmem((slots, chunk, width), f32),
            vmem((every, width), f32),
            vmem((every, width), f32),
            vmem((3, BLOCK, BLOCK), f32),
            vmem((ring, share, BLOCK), f32),
            vmem((ring, 2, share, BLOCK), f32),
            vmem((3, BLOCK, BLOCK), f32),
            vmem((3, share, BLOCK), f32),
            vmem((every, width), f32),
            vmem((every, width), f32),
            vmem((BLOCK, BLOCK), f32),
            vmem((BLOCK, BLOCK), f32),
            vmem((every, width), f32),
            vmem((BLOCK, BLOCK), f32),
            vmem((ring, share, BLOCK), f32),
            vmem((BLOCK, BLOCK), f32),
            vmem((share, BLOCK), f32),
            vmem((near + 1, 2, chunk, width), f32),
            dma((3,)),
            dma,
            dma((2,)),
            dma,
            dma((2,)),
            dma,
            dma((2,)),
            dma,
            dma((5,)),
            dma,
            dma,
            dma,
            dma,
            dma,
            dma,
        ],
        compiler_params=pltpu.CompilerParams(collective_id=0, has_side_effects=True, vmem_limit_bytes=24 * 2**20),
        cost_estimate=pl.CostEstimate(flops=10**9, bytes_accessed=2 * matrix.size * 4, transcendentals=0),
        name="jacobi_steps",
    )(matrix.reshape(chunk, slots, width), plan)
    return result.transpose(1, 0, 2).reshape(matrix.shape)


def solution(mesh):
    in_specs = (P("rows", "cols", None, None), P())
    out_specs = P("rows", "cols", None, None)
    return jax.shard_map(body, mesh=mesh, in_specs=in_specs, out_specs=out_specs, check_vma=False)
```

```python
import functools

import jax
import jax.numpy as jnp
from jax import lax
from jax.experimental import pallas as pl
from jax.experimental.pallas import tpu as pltpu
from jax.sharding import PartitionSpec as P

MESH = pl.DeviceIdType.MESH
XS, ZS, YS, CS = 4, 8, 2, 4
GROUP = XS * YS
BLOCK = 128
WIDTH = 2 * BLOCK
PEERS = ((2, 1), (1, 1), (3, 1), (2, 0), (0, 1), (1, 0), (3, 0))
RING = (4, 3, 5, 2, 6, 1, 7)
FIRST = (((0,), (0,)), ((), ()))
PLAIN = (((1,), (0,)), ((), ()))


def parts_of(value):
    high = value.astype(jnp.bfloat16)
    rest = value - high.astype(jnp.float32)
    middle = rest.astype(jnp.bfloat16)
    low = (rest - middle.astype(jnp.float32)).astype(jnp.bfloat16)
    return high, middle, low


def product(a, b, dims):
    return lax.dot_general(a, b, dims, preferred_element_type=jnp.float32)


def full_product(a, b, dims=PLAIN):
    return lax.dot_general(
        a, b, dims, precision=lax.Precision.HIGHEST, preferred_element_type=jnp.float32
    )


def product_of(a, b, dims=PLAIN):
    high = product(a[0], b[0], dims)
    return high + (product(a[0], b[1], dims) + product(a[1], b[0], dims))


def times_onehot(value, partner):
    rows = lax.broadcasted_iota(jnp.int32, (WIDTH, WIDTH), 0)
    onehot = (rows == partner).astype(jnp.float32).astype(jnp.bfloat16)
    high, middle, low = parts_of(value)
    return product(high, onehot, PLAIN) + (product(middle, onehot, PLAIN) + product(low, onehot, PLAIN))


def turned_by(rotation, partner, cosine, sine):
    if rotation is None:
        below = lax.broadcasted_iota(jnp.int32, (WIDTH, WIDTH), 0)
        along = lax.broadcasted_iota(jnp.int32, (WIDTH, WIDTH), 1)
        return jnp.where(below == along, cosine, 0.0) + jnp.where(below == partner, sine, 0.0)
    return rotation * cosine + times_onehot(rotation, partner) * sine


def columns_moved(value, partner):
    rows = value.shape[0]
    near = jnp.where(partner < BLOCK, partner, partner - BLOCK)
    sides = []
    for half in range(2):
        lanes = slice(half * BLOCK, (half + 1) * BLOCK)
        index = jnp.broadcast_to(near[:, lanes], (rows, BLOCK))
        left = jnp.broadcast_to(partner[:, lanes] < BLOCK, (rows, BLOCK))
        picked = [
            jnp.take_along_axis(value[:, n * BLOCK : (n + 1) * BLOCK], index, axis=1, mode="promise_in_bounds")
            for n in range(2)
        ]
        sides.append(jnp.where(left, picked[0], picked[1]))
    return jnp.concatenate(sides, axis=1)


def solve(gram, plan_of_round, rounds, final_gram, tell):
    below = lax.broadcasted_iota(jnp.int32, (WIDTH, WIDTH), 0)
    along = lax.broadcasted_iota(jnp.int32, (WIDTH, WIDTH), 1)
    unit = below == along
    block_unit = unit[:BLOCK, :BLOCK]
    index = lax.broadcasted_iota(jnp.int32, (1, WIDTH), 1)
    rotation = None
    for r in range(rounds):
        partner = plan_of_round(r)
        pairing = below == partner
        moved = columns_moved(gram, partner)
        own = jnp.concatenate(
            [
                jnp.sum(jnp.where(block_unit, gram[:BLOCK, :BLOCK], 0.0), axis=0, keepdims=True),
                jnp.sum(jnp.where(block_unit, gram[BLOCK:, BLOCK:], 0.0), axis=0, keepdims=True),
            ],
            axis=1,
        )
        cross = jnp.sum(jnp.where(pairing, gram, 0.0), axis=0, keepdims=True)
        other = columns_moved(jnp.broadcast_to(own, (8, WIDTH)), partner)[:1]
        orient = jnp.where(index < partner, 1.0, -1.0)
        spread = orient * (other - own)
        sign = jnp.where(spread >= 0.0, 1.0, -1.0)
        tangent = sign * 2.0 * cross / (jnp.abs(spread) + jnp.sqrt(spread * spread + 4.0 * cross * cross))
        cosine = 1.0 / jnp.sqrt(1.0 + tangent * tangent)
        sine = -orient * (tangent * cosine)
        tell(r, cosine, sine)
        if r + 1 < rounds or final_gram:
            turned = jnp.transpose(gram * cosine + moved * sine)
            gram = turned * cosine + columns_moved(turned, partner) * sine
        rotation = turned_by(rotation, partner, cosine, sine)
    return gram, rotation


def kernel(
    x_hbm,
    plan_hbm,
    result,
    plan_ref,
    x_own,
    tops,
    bottoms,
    partial,
    shares_tt,
    shares_b,
    total,
    total_mine,
    next_tops,
    next_bottoms,
    turns_out,
    turns_in,
    bottoms_in,
    square_out,
    square_in,
    tops_now,
    partial_tb,
    shares_tb,
    total_tb,
    total_tb_mine,
    result_out,
    load_sem,
    in_send,
    in_recv,
    sum_send,
    sum_recv,
    all_send,
    all_recv,
    next_send,
    next_recv,
    sum2_send,
    sum2_recv,
    all2_send,
    all2_recv,
    out_send,
    out_recv,
):
    rows = lax.axis_index("rows")
    col = lax.axis_index("cols")
    x = rows // (ZS * YS)
    z = (rows // YS) % ZS
    y = rows % YS
    me = x * YS + y
    chunk = x_own.shape[1]
    every = tops.shape[0]
    share = BLOCK // ZS
    near, ring = len(PEERS), len(RING)

    def member(a, b):
        return ((x + a) % XS) * YS + (y + b) % YS

    def row_of(a, b):
        return (((x + a) % XS) * ZS + z) * YS + (y + b) % YS

    def ring_row(d):
        return (x * ZS + (z + d) % ZS) * YS + y

    after = (col + 1) % CS
    before = (col + CS - 1) % CS

    def send(src, dst, send_sem, recv_sem, row, column):
        pltpu.make_async_remote_copy(
            src_ref=src, dst_ref=dst, send_sem=send_sem, recv_sem=recv_sem, device_id=(row, column), device_id_type=MESH
        ).start()

    def await_bytes(like, sem):
        pltpu.make_async_remote_copy(
            src_ref=like, dst_ref=like, send_sem=sem, recv_sem=sem, device_id=(rows, col), device_id_type=MESH
        ).wait_recv()

    barrier = pltpu.get_barrier_semaphore()

    def greet(row, column):
        pl.semaphore_signal(barrier, inc=1, device_id=(row, column), device_id_type=MESH)

    for a, b in PEERS:
        greet(row_of(a, b), col)
        greet(row_of(a, b), before)
    greet(rows, before)
    for d in RING:
        greet(ring_row(d), col)

    own_place = pl.ds(pl.multiple_of(me * chunk, chunk), chunk)
    loads = ([], [])
    for half in range(2):
        for a, b in PEERS:
            slot = 2 * member(a, b) + half
            loads[half].append(pltpu.make_async_copy(x_hbm.at[:, slot, :], x_own.at[slot], load_sem.at[half]))
        gathered = (tops, bottoms)[half]
        loads[half].append(pltpu.make_async_copy(x_hbm.at[:, 2 * me + half, :], gathered.at[own_place], load_sem.at[half]))
        for load in loads[half]:
            load.start()
    plan_copy = pltpu.make_async_copy(plan_hbm, plan_ref, load_sem.at[2])
    plan_copy.start()

    pl.semaphore_wait(barrier, 2 * near + 1 + ring)

    for half in range(2):
        gathered = (tops, bottoms)[half]
        for load in loads[half]:
            load.wait()
        for a, b in PEERS:
            send(
                x_own.at[2 * member(a, b) + half],
                gathered.at[own_place],
                in_send,
                in_recv.at[half],
                row_of(a, b),
                col,
            )
    plan_copy.wait()

    def ring_place(d):
        return pl.ds(pl.multiple_of(((z + d) % ZS) * share, share), share)

    await_bytes(tops.at[: near * chunk], in_recv.at[0])
    top_now = tops[...]
    partial[0] = full_product(top_now, top_now, FIRST)
    for n, d in enumerate(RING):
        send(partial.at[0, ring_place(d)], shares_tt.at[n], sum_send, sum_recv.at[0], ring_row(d), col)

    await_bytes(bottoms.at[: near * chunk], in_recv.at[1])
    bottom_now = bottoms[...]
    both = full_product(bottom_now, jnp.concatenate([top_now, bottom_now], axis=1), FIRST)
    partial[1] = both[:, :BLOCK]
    partial[2] = both[:, BLOCK:]
    for n, d in enumerate(RING):
        send(partial.at[1:3, ring_place(d)], shares_b.at[n], sum_send, sum_recv.at[1], ring_row(d), col)

    send(tops, next_tops, next_send, next_recv.at[0], rows, after)
    send(bottoms, next_bottoms, next_send, next_recv.at[1], rows, after)

    here = ring_place(0)
    await_bytes(shares_tt, sum_recv.at[0])
    mine = partial[0, here]
    for n in range(ring):
        mine = mine + shares_tt[n]
    total_mine[0] = mine
    total[0, here] = mine
    for d in RING:
        send(total_mine.at[0], total.at[0, here], all_send, all_recv.at[0], ring_row(d), col)
    await_bytes(shares_b, sum_recv.at[1])
    mine = partial[1:3, here]
    for n in range(ring):
        mine = mine + shares_b[n]
    total_mine[1:3] = mine
    total[1:3, here] = mine
    for d in RING:
        send(total_mine.at[1:3], total.at[1:3, here], all_send, all_recv.at[1], ring_row(d), col)
    await_bytes(next_tops, next_recv.at[0])
    await_bytes(next_bottoms, next_recv.at[1])
    columns = parts_of(jnp.concatenate([top_now, bottom_now], axis=1))
    next_columns = parts_of(jnp.concatenate([next_tops[...], next_bottoms[...]], axis=1))
    between = product_of(columns, next_columns, FIRST)
    await_bytes(total.at[0, : ring * share], all_recv.at[0])
    await_bytes(total.at[1:3, : ring * share], all_recv.at[1])

    cross = total[1]
    gram = jnp.concatenate(
        [jnp.concatenate([total[0], jnp.transpose(cross)], axis=1), jnp.concatenate([cross, total[2]], axis=1)], axis=0
    )
    rounds = plan_ref.shape[1]

    def first_plan(r):
        return plan_ref[0, r : r + 1, :]

    def tell(r, cosine, sine):
        turns_out[r] = jnp.concatenate([cosine, sine], axis=0)
        send(turns_out.at[r], turns_in.at[r], next_send, next_recv.at[2 + r], rows, after)

    gram, rotation = solve(gram, first_plan, rounds, True, tell)
    top_square = gram[:BLOCK, :BLOCK]
    square_out[...] = gram[BLOCK:, BLOCK:]
    send(square_out, square_in, next_send, next_recv.at[2 + rounds], rows, after)

    turns = []
    for r in range(rounds):
        moved = columns_moved(between, first_plan(r))
        await_bytes(turns_in.at[r], next_recv.at[2 + r])
        turns.append((turns_in[r, 0:1, :], turns_in[r, 1:2, :]))
        between = between * turns[r][0] + moved * turns[r][1]
    partial_tb[...] = full_product(rotation[:, :BLOCK], between[:, BLOCK:], FIRST)
    for n, d in enumerate(RING):
        send(partial_tb.at[ring_place(d)], shares_tb.at[n], sum2_send, sum2_recv, ring_row(d), col)
    next_rotation = None
    for r in range(rounds):
        next_rotation = turned_by(next_rotation, first_plan(r), *turns[r])
    bottoms_in[...] = product_of(next_columns, [part[:, BLOCK:] for part in parts_of(next_rotation)])
    tops_now[...] = product_of(columns, [part[:, :BLOCK] for part in parts_of(rotation)])
    await_bytes(shares_tb, sum2_recv)
    mine = partial_tb[here]
    for n in range(ring):
        mine = mine + shares_tb[n]
    total_tb_mine[...] = mine
    total_tb[here] = mine
    for d in RING:
        send(total_tb_mine, total_tb.at[here], all2_send, all2_recv, ring_row(d), col)
    await_bytes(square_in, next_recv.at[2 + rounds])
    await_bytes(total_tb.at[: ring * share], all2_recv)
    cross = total_tb[...]
    gram = jnp.concatenate(
        [jnp.concatenate([top_square, cross], axis=1), jnp.concatenate([jnp.transpose(cross), square_in[...]], axis=1)],
        axis=0,
    )
    _, rotation = solve(gram, lambda r: plan_ref[1, r : r + 1, :], rounds, False, lambda *_: None)

    turn = parts_of(rotation)
    for k, (a, b) in enumerate(PEERS + ((0, 0),)):
        place = pl.ds(pl.multiple_of(member(a, b) * chunk, chunk), chunk)
        now = product_of(parts_of(jnp.concatenate([tops_now[place], bottoms_in[place]], axis=1)), turn)
        result_out[k, 1] = now[:, BLOCK:]
        send(result_out.at[k, 1], result.at[2 * me + 1], out_send, out_recv, row_of(a, b), after)
        if k < near:
            result_out[k, 0] = now[:, :BLOCK]
            send(result_out.at[k, 0], result.at[2 * me], out_send, out_recv, row_of(a, b), col)
        else:
            result[2 * me] = now[:, :BLOCK]
    await_bytes(result.at[: 2 * near + 1], out_recv)
    await_bytes(x_own.at[: 2 * near], in_send)
    await_bytes(tops.at[: 3 * ring * share], sum_send)
    await_bytes(tops.at[: 3 * ring * share], all_send)
    await_bytes(tops, next_send)
    await_bytes(bottoms, next_send)
    await_bytes(turns_out, next_send)
    await_bytes(square_out, next_send)
    await_bytes(shares_tb, sum2_send)
    await_bytes(shares_tb, all2_send)
    await_bytes(result.at[: 2 * near + 1], out_send)


def body(matrix, plan):
    chunk, pairs, halves, width = matrix.shape
    slots = pairs * halves
    every = chunk * GROUP
    share = BLOCK // ZS
    f32 = jnp.float32
    dma = pltpu.SemaphoreType.DMA
    near, ring = len(PEERS), len(RING)
    vmem = pltpu.VMEM
    result = pl.pallas_call(
        kernel,
        out_shape=jax.ShapeDtypeStruct((slots, chunk, width), f32),
        in_specs=[pl.BlockSpec(memory_space=pltpu.HBM)] * 2,
        out_specs=pl.BlockSpec(memory_space=pltpu.VMEM),
        scratch_shapes=[
            vmem(plan.shape, jnp.int32),
            vmem((slots, chunk, width), f32),
            vmem((every, width), f32),
            vmem((every, width), f32),
            vmem((3, BLOCK, BLOCK), f32),
            vmem((ring, share, BLOCK), f32),
            vmem((ring, 2, share, BLOCK), f32),
            vmem((3, BLOCK, BLOCK), f32),
            vmem((3, share, BLOCK), f32),
            vmem((every, width), f32),
            vmem((every, width), f32),
            vmem((plan.shape[1], 2, WIDTH), f32),
            vmem((plan.shape[1], 2, WIDTH), f32),
            vmem((every, width), f32),
            vmem((BLOCK, BLOCK), f32),
            vmem((BLOCK, BLOCK), f32),
            vmem((every, width), f32),
            vmem((BLOCK, BLOCK), f32),
            vmem((ring, share, BLOCK), f32),
            vmem((BLOCK, BLOCK), f32),
            vmem((share, BLOCK), f32),
            vmem((near + 1, 2, chunk, width), f32),
            dma((3,)),
            dma,
            dma((2,)),
            dma,
            dma((2,)),
            dma,
            dma((2,)),
            dma,
            dma((7,)),
            dma,
            dma,
            dma,
            dma,
            dma,
            dma,
        ],
        compiler_params=pltpu.CompilerParams(collective_id=0, has_side_effects=True, vmem_limit_bytes=24 * 2**20),
        cost_estimate=pl.CostEstimate(flops=10**9, bytes_accessed=2 * matrix.size * 4, transcendentals=0),
        name="jacobi_steps",
    )(pltpu.with_memory_space_constraint(matrix.reshape(chunk, slots, width), pltpu.HBM), pltpu.with_memory_space_constraint(plan, pltpu.HBM))
    return result.transpose(1, 0, 2).reshape(matrix.shape)


def solution(mesh):
    in_specs = (P("rows", "cols", None, None), P())
    out_specs = P("rows", "cols", None, None)
    return jax.shard_map(body, mesh=mesh, in_specs=in_specs, out_specs=out_specs, check_vma=False)
```

```python
import functools

import jax
import jax.numpy as jnp
from jax import lax
from jax.experimental import pallas as pl
from jax.experimental.pallas import tpu as pltpu
from jax.sharding import PartitionSpec as P

MESH = pl.DeviceIdType.MESH
XS, ZS, YS, CS = 4, 8, 2, 4
GROUP = XS * YS
BLOCK = 128
WIDTH = 2 * BLOCK
PEERS = ((2, 1), (1, 1), (3, 1), (2, 0), (0, 1), (1, 0), (3, 0))
RING = (4, 3, 5, 2, 6, 1, 7)
FIRST = (((0,), (0,)), ((), ()))
PLAIN = (((1,), (0,)), ((), ()))


def parts_of(value):
    high = value.astype(jnp.bfloat16)
    rest = value - high.astype(jnp.float32)
    middle = rest.astype(jnp.bfloat16)
    low = (rest - middle.astype(jnp.float32)).astype(jnp.bfloat16)
    return high, middle, low


def product(a, b, dims):
    return lax.dot_general(a, b, dims, preferred_element_type=jnp.float32)


def full_product(a, b, dims=PLAIN):
    return lax.dot_general(
        a, b, dims, precision=lax.Precision.HIGHEST, preferred_element_type=jnp.float32
    )


def product_of(a, b, dims=PLAIN):
    high = product(a[0], b[0], dims)
    return high + (product(a[0], b[1], dims) + product(a[1], b[0], dims))


def times_onehot(value, partner):
    rows = lax.broadcasted_iota(jnp.int32, (WIDTH, WIDTH), 0)
    onehot = (rows == partner).astype(jnp.float32).astype(jnp.bfloat16)
    high, middle, low = parts_of(value)
    return product(high, onehot, PLAIN) + (product(middle, onehot, PLAIN) + product(low, onehot, PLAIN))


def turned_by(rotation, partner, cosine, sine):
    if rotation is None:
        below = lax.broadcasted_iota(jnp.int32, (WIDTH, WIDTH), 0)
        along = lax.broadcasted_iota(jnp.int32, (WIDTH, WIDTH), 1)
        return jnp.where(below == along, cosine, 0.0) + jnp.where(below == partner, sine, 0.0)
    return rotation * cosine + times_onehot(rotation, partner) * sine


def columns_moved(value, partner):
    rows = value.shape[0]
    near = jnp.where(partner < BLOCK, partner, partner - BLOCK)
    sides = []
    for half in range(2):
        lanes = slice(half * BLOCK, (half + 1) * BLOCK)
        index = jnp.broadcast_to(near[:, lanes], (rows, BLOCK))
        left = jnp.broadcast_to(partner[:, lanes] < BLOCK, (rows, BLOCK))
        picked = [
            jnp.take_along_axis(value[:, n * BLOCK : (n + 1) * BLOCK], index, axis=1, mode="promise_in_bounds")
            for n in range(2)
        ]
        sides.append(jnp.where(left, picked[0], picked[1]))
    return jnp.concatenate(sides, axis=1)


def solve(gram, plan_of_round, rounds, tell):
    below = lax.broadcasted_iota(jnp.int32, (WIDTH, WIDTH), 0)
    along = lax.broadcasted_iota(jnp.int32, (WIDTH, WIDTH), 1)
    index = lax.broadcasted_iota(jnp.int32, (1, WIDTH), 1)
    rotation = None
    image = gram
    for r in range(rounds):
        partner = plan_of_round(r)
        if r == 0:
            unit = below == along
            pairing = below == partner
            own = jnp.sum(jnp.where(unit, gram, 0.0), axis=0, keepdims=True)
            cross = jnp.sum(jnp.where(pairing, gram, 0.0), axis=0, keepdims=True)
        else:
            own = jnp.sum(rotation * image, axis=0, keepdims=True)
            rotation_moved = columns_moved(rotation, partner)
            cross = jnp.sum(rotation_moved * image, axis=0, keepdims=True)
        other = columns_moved(jnp.broadcast_to(own, (8, WIDTH)), partner)[:1]
        orient = jnp.where(index < partner, 1.0, -1.0)
        spread = orient * (other - own)
        sign = jnp.where(spread >= 0.0, 1.0, -1.0)
        tangent = sign * 2.0 * cross / (jnp.abs(spread) + jnp.sqrt(spread * spread + 4.0 * cross * cross))
        cosine = lax.rsqrt(1.0 + tangent * tangent)
        sine = -orient * (tangent * cosine)
        tell(r, cosine, sine)
        if r == 0:
            rotation = jnp.where(unit, cosine, 0.0) + jnp.where(pairing, sine, 0.0)
        else:
            rotation = rotation * cosine + rotation_moved * sine
        image = image * cosine + columns_moved(image, partner) * sine
    return rotation, image


def kernel(
    x_hbm,
    plan_hbm,
    result,
    plan_ref,
    x_own,
    tops,
    bottoms,
    partial,
    shares_tt,
    shares_b,
    total,
    total_mine,
    next_tops,
    next_bottoms,
    turns_out,
    turns_in,
    bottoms_in,
    square_out,
    square_in,
    tops_now,
    partial_tb,
    shares_tb,
    total_tb,
    total_tb_mine,
    result_out,
    load_sem,
    in_send,
    in_recv,
    sum_send,
    sum_recv,
    all_send,
    all_recv,
    next_send,
    next_recv,
    sum2_send,
    sum2_recv,
    all2_send,
    all2_recv,
    out_send,
    out_recv,
):
    rows = lax.axis_index("rows")
    col = lax.axis_index("cols")
    x = rows // (ZS * YS)
    z = (rows // YS) % ZS
    y = rows % YS
    me = x * YS + y
    chunk = x_own.shape[1]
    every = tops.shape[0]
    share = BLOCK // ZS
    near, ring = len(PEERS), len(RING)

    def member(a, b):
        return ((x + a) % XS) * YS + (y + b) % YS

    def row_of(a, b):
        return (((x + a) % XS) * ZS + z) * YS + (y + b) % YS

    def ring_row(d):
        return (x * ZS + (z + d) % ZS) * YS + y

    after = (col + 1) % CS
    before = (col + CS - 1) % CS

    def send(src, dst, send_sem, recv_sem, row, column):
        pltpu.make_async_remote_copy(
            src_ref=src, dst_ref=dst, send_sem=send_sem, recv_sem=recv_sem, device_id=(row, column), device_id_type=MESH
        ).start()

    def await_bytes(like, sem):
        pltpu.make_async_remote_copy(
            src_ref=like, dst_ref=like, send_sem=sem, recv_sem=sem, device_id=(rows, col), device_id_type=MESH
        ).wait_recv()

    barrier = pltpu.get_barrier_semaphore()

    def greet(row, column):
        pl.semaphore_signal(barrier, inc=1, device_id=(row, column), device_id_type=MESH)

    for a, b in PEERS:
        greet(row_of(a, b), col)
        greet(row_of(a, b), before)
    greet(rows, before)
    for d in RING:
        greet(ring_row(d), col)

    own_place = pl.ds(pl.multiple_of(me * chunk, chunk), chunk)
    loads = ([], [])
    for half in range(2):
        for a, b in PEERS:
            slot = 2 * member(a, b) + half
            loads[half].append(pltpu.make_async_copy(x_hbm.at[:, slot, :], x_own.at[slot], load_sem.at[half]))
        gathered = (tops, bottoms)[half]
        loads[half].append(pltpu.make_async_copy(x_hbm.at[:, 2 * me + half, :], gathered.at[own_place], load_sem.at[half]))
        for load in loads[half]:
            load.start()
    plan_copy = pltpu.make_async_copy(plan_hbm, plan_ref, load_sem.at[2])
    plan_copy.start()

    pl.semaphore_wait(barrier, 2 * near + 1 + ring)

    for half in range(2):
        gathered = (tops, bottoms)[half]
        for load in loads[half]:
            load.wait()
        for a, b in PEERS:
            send(
                x_own.at[2 * member(a, b) + half],
                gathered.at[own_place],
                in_send,
                in_recv.at[half],
                row_of(a, b),
                col,
            )
    plan_copy.wait()

    def ring_place(d):
        return pl.ds(pl.multiple_of(((z + d) % ZS) * share, share), share)

    await_bytes(tops.at[: near * chunk], in_recv.at[0])
    top_now = tops[...]
    partial[0] = full_product(top_now, top_now, FIRST)
    for n, d in enumerate(RING):
        send(partial.at[0, ring_place(d)], shares_tt.at[n], sum_send, sum_recv.at[0], ring_row(d), col)

    await_bytes(bottoms.at[: near * chunk], in_recv.at[1])
    bottom_now = bottoms[...]
    both = full_product(bottom_now, jnp.concatenate([top_now, bottom_now], axis=1), FIRST)
    partial[1] = both[:, :BLOCK]
    partial[2] = both[:, BLOCK:]
    for n, d in enumerate(RING):
        send(partial.at[1:3, ring_place(d)], shares_b.at[n], sum_send, sum_recv.at[1], ring_row(d), col)

    send(tops, next_tops, next_send, next_recv.at[0], rows, after)
    send(bottoms, next_bottoms, next_send, next_recv.at[1], rows, after)

    here = ring_place(0)
    await_bytes(shares_tt, sum_recv.at[0])
    mine = partial[0, here]
    for n in range(ring):
        mine = mine + shares_tt[n]
    total_mine[0] = mine
    total[0, here] = mine
    for d in RING:
        send(total_mine.at[0], total.at[0, here], all_send, all_recv.at[0], ring_row(d), col)
    await_bytes(shares_b, sum_recv.at[1])
    mine = partial[1:3, here]
    for n in range(ring):
        mine = mine + shares_b[n]
    total_mine[1:3] = mine
    total[1:3, here] = mine
    for d in RING:
        send(total_mine.at[1:3], total.at[1:3, here], all_send, all_recv.at[1], ring_row(d), col)
    await_bytes(next_tops, next_recv.at[0])
    await_bytes(next_bottoms, next_recv.at[1])
    columns = parts_of(jnp.concatenate([top_now, bottom_now], axis=1))
    next_columns = parts_of(jnp.concatenate([next_tops[...], next_bottoms[...]], axis=1))
    between = product_of(columns, next_columns, FIRST)
    await_bytes(total.at[0, : ring * share], all_recv.at[0])
    await_bytes(total.at[1:3, : ring * share], all_recv.at[1])

    cross = total[1]
    gram = jnp.concatenate(
        [jnp.concatenate([total[0], jnp.transpose(cross)], axis=1), jnp.concatenate([cross, total[2]], axis=1)], axis=0
    )
    rounds = plan_ref.shape[1]

    def first_plan(r):
        return plan_ref[0, r : r + 1, :]

    def tell(r, cosine, sine):
        turns_out[r] = jnp.concatenate([cosine, sine], axis=0)
        send(turns_out.at[r], turns_in.at[r], next_send, next_recv.at[2 + r], rows, after)

    rotation, image = solve(gram, first_plan, rounds, tell)
    square_out[...] = full_product(rotation[:, BLOCK:], image[:, BLOCK:], FIRST)
    top_square = full_product(rotation[:, :BLOCK], image[:, :BLOCK], FIRST)
    send(square_out, square_in, next_send, next_recv.at[2 + rounds], rows, after)

    turns = []
    for r in range(rounds):
        moved = columns_moved(between, first_plan(r))
        await_bytes(turns_in.at[r], next_recv.at[2 + r])
        turns.append((turns_in[r, 0:1, :], turns_in[r, 1:2, :]))
        between = between * turns[r][0] + moved * turns[r][1]
    partial_tb[...] = full_product(rotation[:, :BLOCK], between[:, BLOCK:], FIRST)
    for n, d in enumerate(RING):
        send(partial_tb.at[ring_place(d)], shares_tb.at[n], sum2_send, sum2_recv, ring_row(d), col)
    next_rotation = None
    for r in range(rounds):
        next_rotation = turned_by(next_rotation, first_plan(r), *turns[r])
    bottoms_in[...] = product_of(next_columns, [part[:, BLOCK:] for part in parts_of(next_rotation)])
    tops_now[...] = product_of(columns, [part[:, :BLOCK] for part in parts_of(rotation)])
    await_bytes(shares_tb, sum2_recv)
    mine = partial_tb[here]
    for n in range(ring):
        mine = mine + shares_tb[n]
    total_tb_mine[...] = mine
    total_tb[here] = mine
    for d in RING:
        send(total_tb_mine, total_tb.at[here], all2_send, all2_recv, ring_row(d), col)
    await_bytes(square_in, next_recv.at[2 + rounds])
    await_bytes(total_tb.at[: ring * share], all2_recv)
    cross = total_tb[...]
    gram = jnp.concatenate(
        [jnp.concatenate([top_square, cross], axis=1), jnp.concatenate([jnp.transpose(cross), square_in[...]], axis=1)],
        axis=0,
    )
    rotation, _ = solve(gram, lambda r: plan_ref[1, r : r + 1, :], rounds, lambda *_: None)

    turn = parts_of(rotation)
    for k, (a, b) in enumerate(PEERS + ((0, 0),)):
        place = pl.ds(pl.multiple_of(member(a, b) * chunk, chunk), chunk)
        now = product_of(parts_of(jnp.concatenate([tops_now[place], bottoms_in[place]], axis=1)), turn)
        result_out[k, 1] = now[:, BLOCK:]
        send(result_out.at[k, 1], result.at[2 * me + 1], out_send, out_recv, row_of(a, b), after)
        if k < near:
            result_out[k, 0] = now[:, :BLOCK]
            send(result_out.at[k, 0], result.at[2 * me], out_send, out_recv, row_of(a, b), col)
        else:
            result[2 * me] = now[:, :BLOCK]
    await_bytes(result.at[: 2 * near + 1], out_recv)
    await_bytes(x_own.at[: 2 * near], in_send)
    await_bytes(tops.at[: 3 * ring * share], sum_send)
    await_bytes(tops.at[: 3 * ring * share], all_send)
    await_bytes(tops, next_send)
    await_bytes(bottoms, next_send)
    await_bytes(turns_out, next_send)
    await_bytes(square_out, next_send)
    await_bytes(shares_tb, sum2_send)
    await_bytes(shares_tb, all2_send)
    await_bytes(result.at[: 2 * near + 1], out_send)


def body(matrix, plan):
    chunk, pairs, halves, width = matrix.shape
    slots = pairs * halves
    every = chunk * GROUP
    share = BLOCK // ZS
    f32 = jnp.float32
    dma = pltpu.SemaphoreType.DMA
    near, ring = len(PEERS), len(RING)
    vmem = pltpu.VMEM
    result = pl.pallas_call(
        kernel,
        out_shape=jax.ShapeDtypeStruct((slots, chunk, width), f32),
        in_specs=[pl.BlockSpec(memory_space=pltpu.HBM)] * 2,
        out_specs=pl.BlockSpec(memory_space=pltpu.VMEM),
        scratch_shapes=[
            vmem(plan.shape, jnp.int32),
            vmem((slots, chunk, width), f32),
            vmem((every, width), f32),
            vmem((every, width), f32),
            vmem((3, BLOCK, BLOCK), f32),
            vmem((ring, share, BLOCK), f32),
            vmem((ring, 2, share, BLOCK), f32),
            vmem((3, BLOCK, BLOCK), f32),
            vmem((3, share, BLOCK), f32),
            vmem((every, width), f32),
            vmem((every, width), f32),
            vmem((plan.shape[1], 2, WIDTH), f32),
            vmem((plan.shape[1], 2, WIDTH), f32),
            vmem((every, width), f32),
            vmem((BLOCK, BLOCK), f32),
            vmem((BLOCK, BLOCK), f32),
            vmem((every, width), f32),
            vmem((BLOCK, BLOCK), f32),
            vmem((ring, share, BLOCK), f32),
            vmem((BLOCK, BLOCK), f32),
            vmem((share, BLOCK), f32),
            vmem((near + 1, 2, chunk, width), f32),
            dma((3,)),
            dma,
            dma((2,)),
            dma,
            dma((2,)),
            dma,
            dma((2,)),
            dma,
            dma((7,)),
            dma,
            dma,
            dma,
            dma,
            dma,
            dma,
        ],
        compiler_params=pltpu.CompilerParams(collective_id=0, has_side_effects=True, vmem_limit_bytes=24 * 2**20),
        cost_estimate=pl.CostEstimate(flops=10**9, bytes_accessed=2 * matrix.size * 4, transcendentals=0),
        name="jacobi_steps",
    )(pltpu.with_memory_space_constraint(matrix.reshape(chunk, slots, width), pltpu.HBM), pltpu.with_memory_space_constraint(plan, pltpu.HBM))
    return result.transpose(1, 0, 2).reshape(matrix.shape)


def solution(mesh):
    in_specs = (P("rows", "cols", None, None), P())
    out_specs = P("rows", "cols", None, None)
    return jax.shard_map(body, mesh=mesh, in_specs=in_specs, out_specs=out_specs, check_vma=False)
```

```python
import functools

import jax
import jax.numpy as jnp
from jax import lax
from jax.experimental import pallas as pl
from jax.experimental.pallas import tpu as pltpu
from jax.sharding import PartitionSpec as P

MESH = pl.DeviceIdType.MESH
XS, ZS, YS, CS = 4, 8, 2, 4
GROUP = XS * YS
BLOCK = 128
WIDTH = 2 * BLOCK
PEERS = ((2, 1), (0, 1), (1, 1), (2, 0), (3, 1), (1, 0), (3, 0))
RING = (4, 3, 5, 2, 6, 1, 7)
FIRST = (((0,), (0,)), ((), ()))
PLAIN = (((1,), (0,)), ((), ()))


def parts_of(value):
    high = value.astype(jnp.bfloat16)
    rest = value - high.astype(jnp.float32)
    middle = rest.astype(jnp.bfloat16)
    low = (rest - middle.astype(jnp.float32)).astype(jnp.bfloat16)
    return high, middle, low


def product(a, b, dims):
    return lax.dot_general(a, b, dims, preferred_element_type=jnp.float32)


def full_product(a, b, dims=PLAIN):
    return lax.dot_general(
        a, b, dims, precision=lax.Precision.HIGHEST, preferred_element_type=jnp.float32
    )


def product_of(a, b, dims=PLAIN):
    high = product(a[0], b[0], dims)
    return high + (product(a[0], b[1], dims) + product(a[1], b[0], dims))


def times_onehot(value, partner):
    rows = lax.broadcasted_iota(jnp.int32, (WIDTH, WIDTH), 0)
    onehot = (rows == partner).astype(jnp.float32).astype(jnp.bfloat16)
    high, middle, low = parts_of(value)
    return product(high, onehot, PLAIN) + (product(middle, onehot, PLAIN) + product(low, onehot, PLAIN))


def turned_by(rotation, partner, cosine, sine):
    if rotation is None:
        below = lax.broadcasted_iota(jnp.int32, (WIDTH, WIDTH), 0)
        along = lax.broadcasted_iota(jnp.int32, (WIDTH, WIDTH), 1)
        return jnp.where(below == along, cosine, 0.0) + jnp.where(below == partner, sine, 0.0)
    return rotation * cosine + times_onehot(rotation, partner) * sine


def columns_moved(value, partner):
    rows = value.shape[0]
    near = jnp.where(partner < BLOCK, partner, partner - BLOCK)
    sides = []
    for half in range(2):
        lanes = slice(half * BLOCK, (half + 1) * BLOCK)
        index = jnp.broadcast_to(near[:, lanes], (rows, BLOCK))
        left = jnp.broadcast_to(partner[:, lanes] < BLOCK, (rows, BLOCK))
        picked = [
            jnp.take_along_axis(value[:, n * BLOCK : (n + 1) * BLOCK], index, axis=1, mode="promise_in_bounds")
            for n in range(2)
        ]
        sides.append(jnp.where(left, picked[0], picked[1]))
    return jnp.concatenate(sides, axis=1)


def solve(gram, plan_of_round, rounds, tell):
    below = lax.broadcasted_iota(jnp.int32, (WIDTH, WIDTH), 0)
    along = lax.broadcasted_iota(jnp.int32, (WIDTH, WIDTH), 1)
    index = lax.broadcasted_iota(jnp.int32, (1, WIDTH), 1)
    rotation = None
    image = gram
    for r in range(rounds):
        partner = plan_of_round(r)
        if r == 0:
            unit = below == along
            pairing = below == partner
            own = jnp.sum(jnp.where(unit, gram, 0.0), axis=0, keepdims=True)
            cross = jnp.sum(jnp.where(pairing, gram, 0.0), axis=0, keepdims=True)
        else:
            own = jnp.sum(rotation * image, axis=0, keepdims=True)
            rotation_moved = columns_moved(rotation, partner)
            cross = jnp.sum(rotation_moved * image, axis=0, keepdims=True)
        other = columns_moved(jnp.broadcast_to(own, (8, WIDTH)), partner)[:1]
        orient = jnp.where(index < partner, 1.0, -1.0)
        spread = orient * (other - own)
        sign = jnp.where(spread >= 0.0, 1.0, -1.0)
        tangent = sign * 2.0 * cross / (jnp.abs(spread) + jnp.sqrt(spread * spread + 4.0 * cross * cross))
        cosine = lax.rsqrt(1.0 + tangent * tangent)
        sine = -orient * (tangent * cosine)
        tell(r, cosine, sine)
        if r == 0:
            rotation = jnp.where(unit, cosine, 0.0) + jnp.where(pairing, sine, 0.0)
        else:
            rotation = rotation * cosine + rotation_moved * sine
        image = image * cosine + columns_moved(image, partner) * sine
    return rotation, image


def kernel(
    x_hbm,
    plan_hbm,
    result,
    plan_ref,
    x_own,
    tops,
    bottoms,
    partial,
    shares_tt,
    shares_b,
    total,
    total_mine,
    next_tops,
    next_bottoms,
    turns_out,
    turns_in,
    bottoms_in,
    square_out,
    square_in,
    tops_now,
    partial_tb,
    shares_tb,
    total_tb,
    total_tb_mine,
    result_out,
    load_sem,
    in_send,
    in_recv,
    sum_send,
    sum_recv,
    all_send,
    all_recv,
    next_send,
    next_recv,
    sum2_send,
    sum2_recv,
    all2_send,
    all2_recv,
    out_send,
    out_recv,
):
    rows = lax.axis_index("rows")
    col = lax.axis_index("cols")
    x = rows // (ZS * YS)
    z = (rows // YS) % ZS
    y = rows % YS
    me = x * YS + y
    chunk = x_own.shape[1]
    every = tops.shape[0]
    share = BLOCK // ZS
    near, ring = len(PEERS), len(RING)

    def member(a, b):
        return ((x + a) % XS) * YS + (y + b) % YS

    def row_of(a, b):
        return (((x + a) % XS) * ZS + z) * YS + (y + b) % YS

    def ring_row(d):
        return (x * ZS + (z + d) % ZS) * YS + y

    lane = col % 2
    other_lane = 1 - lane
    base = col - lane
    adds = lane == 1

    def by_core(adding, plain):
        pl.when(adds)(adding)
        pl.when(jnp.logical_not(adds))(plain)

    after = (col + 1) % CS
    before = (col + CS - 1) % CS

    def send(src, dst, send_sem, recv_sem, row, column):
        pltpu.make_async_remote_copy(
            src_ref=src, dst_ref=dst, send_sem=send_sem, recv_sem=recv_sem, device_id=(row, column), device_id_type=MESH
        ).start()

    def await_bytes(like, sem):
        pltpu.make_async_remote_copy(
            src_ref=like, dst_ref=like, send_sem=sem, recv_sem=sem, device_id=(rows, col), device_id_type=MESH
        ).wait_recv()

    barrier = pltpu.get_barrier_semaphore()

    def greet(row, column):
        pl.semaphore_signal(barrier, inc=1, device_id=(row, column), device_id_type=MESH)

    for a, b in PEERS:
        greet(row_of(a, b), col)
        greet(row_of(a, b), before)
    greet(rows, before)
    for d in RING:
        greet(ring_row(d), base)
        greet(ring_row(d), base + 1)
    greet(rows, base + other_lane)

    own_place = pl.ds(pl.multiple_of(me * chunk, chunk), chunk)
    loads = ([], [])
    for half in range(2):
        for a, b in PEERS:
            slot = 2 * member(a, b) + half
            loads[half].append(pltpu.make_async_copy(x_hbm.at[:, slot, :], x_own.at[slot], load_sem.at[half]))
        gathered = (tops, bottoms)[half]
        loads[half].append(pltpu.make_async_copy(x_hbm.at[:, 2 * me + half, :], gathered.at[own_place], load_sem.at[half]))
        for load in loads[half]:
            load.start()
    plan_copy = pltpu.make_async_copy(plan_hbm, plan_ref, load_sem.at[2])
    plan_copy.start()

    pl.semaphore_wait(barrier, 2 * near + 1 + 2 * ring + 1)

    for half in range(2):
        gathered = (tops, bottoms)[half]
        for load in loads[half]:
            load.wait()
        for a, b in PEERS:
            send(
                x_own.at[2 * member(a, b) + half],
                gathered.at[own_place],
                in_send,
                in_recv.at[half],
                row_of(a, b),
                col,
            )
    plan_copy.wait()

    def ring_place(d):
        return pl.ds(pl.multiple_of(((z + d) % ZS) * share, share), share)

    here = ring_place(0)

    def scatter(take, slots, send_sem, recv_sems):
        for n, d in enumerate(RING):
            send(take(ring_place(d)), slots.at[lane, n], send_sem, recv_sems.at[lane], ring_row(d), base + 1)

        @pl.when(jnp.logical_not(adds))
        def _():
            send(take(here), slots.at[0, ring], send_sem, recv_sems.at[0], rows, base + 1)

    def gather(core, mine, home, send_sem, recv_sem):
        for d in RING:
            send(mine, home, send_sem, recv_sem, ring_row(d), base + core)
        if core == 0:
            send(mine, home, send_sem, recv_sem, rows, base)

    await_bytes(tops.at[: near * chunk], in_recv.at[0])
    top_now = tops[...]
    partial[0] = full_product(top_now, top_now, FIRST)
    scatter(lambda place: partial.at[0:1, place], shares_tt, sum_send, sum_recv.at[0])

    await_bytes(bottoms.at[: near * chunk], in_recv.at[1])
    bottom_now = bottoms[...]
    both = full_product(bottom_now, jnp.concatenate([top_now, bottom_now], axis=1), FIRST)
    partial[1] = both[:, :BLOCK]
    partial[2] = both[:, BLOCK:]
    scatter(lambda place: partial.at[1:3, place], shares_b, sum_send, sum_recv.at[1])

    send(tops, next_tops, next_send, next_recv.at[0], rows, after)
    send(bottoms, next_bottoms, next_send, next_recv.at[1], rows, after)

    @pl.when(adds)
    def _():
        for block, slots in ((slice(0, 1), shares_tt), (slice(1, 3), shares_b)):
            n_sem = block.start
            await_bytes(slots.at[1, :ring], sum_recv.at[n_sem, 1])
            mine = partial[block, here]
            for n in range(ring):
                mine = mine + slots[1, n].reshape(mine.shape)
            total_mine[1, block] = mine
            total[block, here] = mine
            gather(1, total_mine.at[1, block], total.at[block, here], all_send, all_recv.at[n_sem])
            await_bytes(slots.at[0], sum_recv.at[n_sem, 0])
            mine = slots[0, 0].reshape(mine.shape)
            for n in range(1, ring + 1):
                mine = mine + slots[0, n].reshape(mine.shape)
            total_mine[0, block] = mine
            gather(0, total_mine.at[0, block], total.at[block, here], all_send, all_recv.at[n_sem])

    await_bytes(next_tops, next_recv.at[0])
    await_bytes(next_bottoms, next_recv.at[1])
    columns = parts_of(jnp.concatenate([top_now, bottom_now], axis=1))
    next_columns = parts_of(jnp.concatenate([next_tops[...], next_bottoms[...]], axis=1))
    between = product_of(columns, next_columns, FIRST)
    def adding():
        await_bytes(total.at[0:1, : ring * share], all_recv.at[0])
        await_bytes(total.at[1:3, : ring * share], all_recv.at[1])

    def plain():
        await_bytes(total.at[0:1], all_recv.at[0])
        await_bytes(total.at[1:3], all_recv.at[1])

    by_core(adding, plain)

    cross = total[1]
    gram = jnp.concatenate(
        [jnp.concatenate([total[0], jnp.transpose(cross)], axis=1), jnp.concatenate([cross, total[2]], axis=1)], axis=0
    )
    rounds = plan_ref.shape[1]

    def first_plan(r):
        return plan_ref[0, r : r + 1, :]

    def tell(r, cosine, sine):
        turns_out[r] = jnp.concatenate([cosine, sine], axis=0)
        send(turns_out.at[r], turns_in.at[r], next_send, next_recv.at[2 + r], rows, after)

    rotation, image = solve(gram, first_plan, rounds, tell)
    square_out[...] = full_product(rotation[:, BLOCK:], image[:, BLOCK:], FIRST)
    top_square = full_product(rotation[:, :BLOCK], image[:, :BLOCK], FIRST)
    send(square_out, square_in, next_send, next_recv.at[2 + rounds], rows, after)

    turns = []
    for r in range(rounds):
        moved = columns_moved(between, first_plan(r))
        await_bytes(turns_in.at[r], next_recv.at[2 + r])
        turns.append((turns_in[r, 0:1, :], turns_in[r, 1:2, :]))
        between = between * turns[r][0] + moved * turns[r][1]
    partial_tb[...] = full_product(rotation[:, :BLOCK], between[:, BLOCK:], FIRST)
    scatter(lambda place: partial_tb.at[place], shares_tb, sum2_send, sum2_recv)
    next_rotation = None
    for r in range(rounds):
        next_rotation = turned_by(next_rotation, first_plan(r), *turns[r])
    bottoms_in[...] = product_of(next_columns, [part[:, BLOCK:] for part in parts_of(next_rotation)])
    tops_now[...] = product_of(columns, [part[:, :BLOCK] for part in parts_of(rotation)])
    @pl.when(adds)
    def _():
        await_bytes(shares_tb.at[1, :ring], sum2_recv.at[1])
        mine = partial_tb[here]
        for n in range(ring):
            mine = mine + shares_tb[1, n]
        total_tb_mine[1] = mine
        total_tb[here] = mine
        gather(1, total_tb_mine.at[1], total_tb.at[here], all2_send, all2_recv)
        await_bytes(shares_tb.at[0], sum2_recv.at[0])
        mine = shares_tb[0, 0]
        for n in range(1, ring + 1):
            mine = mine + shares_tb[0, n]
        total_tb_mine[0] = mine
        gather(0, total_tb_mine.at[0], total_tb.at[here], all2_send, all2_recv)

    await_bytes(square_in, next_recv.at[2 + rounds])
    by_core(lambda: await_bytes(total_tb.at[: ring * share], all2_recv), lambda: await_bytes(total_tb, all2_recv))
    cross = total_tb[...]
    gram = jnp.concatenate(
        [jnp.concatenate([top_square, cross], axis=1), jnp.concatenate([jnp.transpose(cross), square_in[...]], axis=1)],
        axis=0,
    )
    rotation, _ = solve(gram, lambda r: plan_ref[1, r : r + 1, :], rounds, lambda *_: None)

    turn = parts_of(rotation)
    for k, (a, b) in enumerate(PEERS + ((0, 0),)):
        place = pl.ds(pl.multiple_of(member(a, b) * chunk, chunk), chunk)
        now = product_of(parts_of(jnp.concatenate([tops_now[place], bottoms_in[place]], axis=1)), turn)
        result_out[k, 1] = now[:, BLOCK:]
        send(result_out.at[k, 1], result.at[2 * me + 1], out_send, out_recv, row_of(a, b), after)
        if k < near:
            result_out[k, 0] = now[:, :BLOCK]
            send(result_out.at[k, 0], result.at[2 * me], out_send, out_recv, row_of(a, b), col)
        else:
            result[2 * me] = now[:, :BLOCK]
    await_bytes(result.at[: 2 * near + 1], out_recv)
    await_bytes(x_own.at[: 2 * near], in_send)

    def adding():
        await_bytes(tops.at[: 3 * ring * share], sum_send)
        for _ in range(3):
            await_bytes(tops.at[: (2 * ring + 1) * share], all_send)
        await_bytes(tops.at[: ring * share], sum2_send)
        await_bytes(tops.at[: (2 * ring + 1) * share], all2_send)

    def plain():
        await_bytes(tops.at[: 3 * ZS * share], sum_send)
        await_bytes(tops.at[: ZS * share], sum2_send)

    by_core(adding, plain)
    await_bytes(tops, next_send)
    await_bytes(bottoms, next_send)
    await_bytes(turns_out, next_send)
    await_bytes(square_out, next_send)
    await_bytes(result.at[: 2 * near + 1], out_send)


def body(matrix, plan):
    chunk, pairs, halves, width = matrix.shape
    slots = pairs * halves
    every = chunk * GROUP
    share = BLOCK // ZS
    f32 = jnp.float32
    dma = pltpu.SemaphoreType.DMA
    near, ring = len(PEERS), len(RING)
    vmem = pltpu.VMEM
    result = pl.pallas_call(
        kernel,
        out_shape=jax.ShapeDtypeStruct((slots, chunk, width), f32),
        in_specs=[pl.BlockSpec(memory_space=pltpu.HBM)] * 2,
        out_specs=pl.BlockSpec(memory_space=pltpu.VMEM),
        scratch_shapes=[
            vmem(plan.shape, jnp.int32),
            vmem((slots, chunk, width), f32),
            vmem((every, width), f32),
            vmem((every, width), f32),
            vmem((3, BLOCK, BLOCK), f32),
            vmem((2, ZS, 1, share, BLOCK), f32),
            vmem((2, ZS, 2, share, BLOCK), f32),
            vmem((3, BLOCK, BLOCK), f32),
            vmem((2, 3, share, BLOCK), f32),
            vmem((every, width), f32),
            vmem((every, width), f32),
            vmem((plan.shape[1], 2, WIDTH), f32),
            vmem((plan.shape[1], 2, WIDTH), f32),
            vmem((every, width), f32),
            vmem((BLOCK, BLOCK), f32),
            vmem((BLOCK, BLOCK), f32),
            vmem((every, width), f32),
            vmem((BLOCK, BLOCK), f32),
            vmem((2, ZS, share, BLOCK), f32),
            vmem((BLOCK, BLOCK), f32),
            vmem((2, share, BLOCK), f32),
            vmem((near + 1, 2, chunk, width), f32),
            dma((3,)),
            dma,
            dma((2,)),
            dma,
            dma((2, 2)),
            dma,
            dma((2,)),
            dma,
            dma((7,)),
            dma,
            dma((2,)),
            dma,
            dma,
            dma,
            dma,
        ],
        compiler_params=pltpu.CompilerParams(collective_id=0, has_side_effects=True, vmem_limit_bytes=24 * 2**20),
        cost_estimate=pl.CostEstimate(flops=10**9, bytes_accessed=2 * matrix.size * 4, transcendentals=0),
        name="jacobi_steps",
    )(pltpu.with_memory_space_constraint(matrix.reshape(chunk, slots, width), pltpu.HBM), pltpu.with_memory_space_constraint(plan, pltpu.HBM))
    return result.transpose(1, 0, 2).reshape(matrix.shape)


def solution(mesh):
    in_specs = (P("rows", "cols", None, None), P())
    out_specs = P("rows", "cols", None, None)
    return jax.shard_map(body, mesh=mesh, in_specs=in_specs, out_specs=out_specs, check_vma=False)
```

```python
import functools

import jax
import jax.numpy as jnp
from jax import lax
from jax.experimental import pallas as pl
from jax.experimental.pallas import tpu as pltpu
from jax.sharding import PartitionSpec as P

MESH = pl.DeviceIdType.MESH
XS, ZS, YS, CS = 4, 8, 2, 4
GROUP = XS * YS
BLOCK = 128
WIDTH = 2 * BLOCK
PEERS = ((2, 1), (0, 1), (1, 1), (2, 0), (3, 1), (1, 0), (3, 0))
RING = (4, 3, 5, 2, 6, 1, 7)
FIRST = (((0,), (0,)), ((), ()))
PLAIN = (((1,), (0,)), ((), ()))


def parts_of(value):
    high = value.astype(jnp.bfloat16)
    rest = value - high.astype(jnp.float32)
    middle = rest.astype(jnp.bfloat16)
    low = (rest - middle.astype(jnp.float32)).astype(jnp.bfloat16)
    return high, middle, low


def product(a, b, dims):
    return lax.dot_general(a, b, dims, preferred_element_type=jnp.float32)


def full_product(a, b, dims=PLAIN):
    return lax.dot_general(
        a, b, dims, precision=lax.Precision.HIGHEST, preferred_element_type=jnp.float32
    )


def product_of(a, b, dims=PLAIN):
    high = product(a[0], b[0], dims)
    return high + (product(a[0], b[1], dims) + product(a[1], b[0], dims))


def times_onehot(value, partner):
    rows = lax.broadcasted_iota(jnp.int32, (WIDTH, WIDTH), 0)
    onehot = (rows == partner).astype(jnp.float32).astype(jnp.bfloat16)
    high, middle, low = parts_of(value)
    return product(high, onehot, PLAIN) + (product(middle, onehot, PLAIN) + product(low, onehot, PLAIN))


def turned_by(rotation, partner, cosine, sine):
    if rotation is None:
        below = lax.broadcasted_iota(jnp.int32, (WIDTH, WIDTH), 0)
        along = lax.broadcasted_iota(jnp.int32, (WIDTH, WIDTH), 1)
        return jnp.where(below == along, cosine, 0.0) + jnp.where(below == partner, sine, 0.0)
    return rotation * cosine + times_onehot(rotation, partner) * sine


def columns_moved(value, partner):
    rows = value.shape[0]
    near = jnp.where(partner < BLOCK, partner, partner - BLOCK)
    sides = []
    for half in range(2):
        lanes = slice(half * BLOCK, (half + 1) * BLOCK)
        index = jnp.broadcast_to(near[:, lanes], (rows, BLOCK))
        left = jnp.broadcast_to(partner[:, lanes] < BLOCK, (rows, BLOCK))
        picked = [
            jnp.take_along_axis(value[:, n * BLOCK : (n + 1) * BLOCK], index, axis=1, mode="promise_in_bounds")
            for n in range(2)
        ]
        sides.append(jnp.where(left, picked[0], picked[1]))
    return jnp.concatenate(sides, axis=1)


def solve(gram, plan_of_round, rounds, tell):
    below = lax.broadcasted_iota(jnp.int32, (WIDTH, WIDTH), 0)
    along = lax.broadcasted_iota(jnp.int32, (WIDTH, WIDTH), 1)
    index = lax.broadcasted_iota(jnp.int32, (1, WIDTH), 1)
    rotation = None
    image = gram
    for r in range(rounds):
        partner = plan_of_round(r)
        if r == 0:
            unit = below == along
            pairing = below == partner
            own = jnp.sum(jnp.where(unit, gram, 0.0), axis=0, keepdims=True)
            cross = jnp.sum(jnp.where(pairing, gram, 0.0), axis=0, keepdims=True)
        else:
            own = jnp.sum(rotation * image, axis=0, keepdims=True)
            rotation_moved = columns_moved(rotation, partner)
            cross = jnp.sum(rotation_moved * image, axis=0, keepdims=True)
        other = columns_moved(jnp.broadcast_to(own, (8, WIDTH)), partner)[:1]
        orient = jnp.where(index < partner, 1.0, -1.0)
        spread = orient * (other - own)
        sign = jnp.where(spread >= 0.0, 1.0, -1.0)
        tangent = sign * 2.0 * cross / (jnp.abs(spread) + jnp.sqrt(spread * spread + 4.0 * cross * cross))
        cosine = lax.rsqrt(1.0 + tangent * tangent)
        sine = -orient * (tangent * cosine)
        tell(r, cosine, sine)
        if r == 0:
            rotation = jnp.where(unit, cosine, 0.0) + jnp.where(pairing, sine, 0.0)
        else:
            rotation = rotation * cosine + rotation_moved * sine
        image = image * cosine + columns_moved(image, partner) * sine
    return rotation, image


def kernel(
    x_hbm,
    plan_hbm,
    result,
    plan_ref,
    x_own,
    tops,
    bottoms,
    partial,
    shares_tt,
    shares_b,
    total,
    total_mine,
    next_tops,
    next_bottoms,
    turns_out,
    turns_in,
    bottoms_in,
    square_out,
    square_in,
    tops_now,
    between,
    shares_c,
    half_turned,
    half_turned_mine,
    result_out,
    load_sem,
    in_send,
    in_recv,
    sum_send,
    sum_recv,
    all_send,
    all_recv,
    next_send,
    next_recv,
    cross_send,
    cross_recv,
    all2_send,
    all2_recv,
    out_send,
    out_recv,
):
    rows = lax.axis_index("rows")
    col = lax.axis_index("cols")
    x = rows // (ZS * YS)
    z = (rows // YS) % ZS
    y = rows % YS
    me = x * YS + y
    chunk = x_own.shape[1]
    every = tops.shape[0]
    share = BLOCK // ZS
    near, ring = len(PEERS), len(RING)
    early = near // 2

    def member(a, b):
        return ((x + a) % XS) * YS + (y + b) % YS

    def row_of(a, b):
        return (((x + a) % XS) * ZS + z) * YS + (y + b) % YS

    def ring_row(d):
        return (x * ZS + (z + d) % ZS) * YS + y

    after = (col + 1) % CS
    before = (col + CS - 1) % CS

    def send(src, dst, send_sem, recv_sem, row, column):
        pltpu.make_async_remote_copy(
            src_ref=src, dst_ref=dst, send_sem=send_sem, recv_sem=recv_sem, device_id=(row, column), device_id_type=MESH
        ).start()

    def await_bytes(like, sem):
        pltpu.make_async_remote_copy(
            src_ref=like, dst_ref=like, send_sem=sem, recv_sem=sem, device_id=(rows, col), device_id_type=MESH
        ).wait_recv()

    barrier = pltpu.get_barrier_semaphore()

    def greet(row, column):
        pl.semaphore_signal(barrier, inc=1, device_id=(row, column), device_id_type=MESH)

    for a, b in PEERS:
        greet(row_of(a, b), col)
        greet(row_of(a, b), before)
    greet(rows, before)
    for d in RING:
        greet(ring_row(d), col)

    own_place = pl.ds(pl.multiple_of(me * chunk, chunk), chunk)
    loads = ([], [])
    for half in range(2):
        for a, b in PEERS:
            slot = 2 * member(a, b) + half
            loads[half].append(pltpu.make_async_copy(x_hbm.at[:, slot, :], x_own.at[slot], load_sem.at[half]))
        gathered = (tops, bottoms)[half]
        loads[half].append(pltpu.make_async_copy(x_hbm.at[:, 2 * me + half, :], gathered.at[own_place], load_sem.at[half]))
        for load in loads[half]:
            load.start()
    plan_copy = pltpu.make_async_copy(plan_hbm, plan_ref, load_sem.at[2])
    plan_copy.start()

    pl.delay(1)
    pl.semaphore_wait(barrier, 2 * near + 1 + ring)

    pl.delay(1)
    for half in range(2):
        gathered = (tops, bottoms)[half]
        for load in loads[half]:
            load.wait()
        for k, (a, b) in enumerate(PEERS):
            send(
                x_own.at[2 * member(a, b) + half],
                gathered.at[own_place],
                in_send,
                in_recv.at[half, int(k >= early)],
                row_of(a, b),
                col,
            )
    plan_copy.wait()

    def ring_place(d):
        return pl.ds(pl.multiple_of(((z + d) % ZS) * share, share), share)

    pl.delay(1)
    def lines_of(gathered, batch):
        offsets = ((0, 0), *PEERS[:early]) if batch == 0 else PEERS[early:]
        places = [pl.ds(pl.multiple_of(member(XS - a, YS - b) * chunk, chunk), chunk) for a, b in offsets]
        return jnp.concatenate([gathered[place] for place in places], axis=0)

    def arrived(gathered, half, batch):
        count = near - early if batch else early
        await_bytes(gathered.at[: count * chunk], in_recv.at[half, batch])

    arrived(tops, 0, 0)
    tops_early = lines_of(tops, 0)
    square_early = full_product(tops_early, tops_early, FIRST)
    arrived(tops, 0, 1)
    pl.delay(1)
    @pl.when(col % 2 == 0)
    def _():
        send(tops, next_tops, next_send, next_recv.at[0], rows, after)

    tops_late = lines_of(tops, 1)
    partial[0] = square_early + full_product(tops_late, tops_late, FIRST)
    for n, d in enumerate(RING):
        send(partial.at[0, ring_place(d)], shares_tt.at[n], sum_send, sum_recv.at[0], ring_row(d), col)

    pl.delay(1)
    arrived(bottoms, 1, 0)
    bottoms_early = lines_of(bottoms, 0)
    both_early = full_product(bottoms_early, jnp.concatenate([tops_early, bottoms_early], axis=1), FIRST)
    arrived(bottoms, 1, 1)
    pl.delay(1)
    bottoms_late = lines_of(bottoms, 1)
    both = both_early + full_product(bottoms_late, jnp.concatenate([tops_late, bottoms_late], axis=1), FIRST)
    partial[1] = both[:, :BLOCK]
    partial[2] = both[:, BLOCK:]
    for n, d in enumerate(RING):
        send(partial.at[1:3, ring_place(d)], shares_b.at[n], sum_send, sum_recv.at[1], ring_row(d), col)

    @pl.when(col % 2 == 1)
    def _():
        send(tops, next_tops, next_send, next_recv.at[0], rows, after)

    send(bottoms, next_bottoms, next_send, next_recv.at[1], rows, after)

    def cross_products(half):
        arrived_block = (next_tops, next_bottoms)[half]
        await_bytes(arrived_block, next_recv.at[half])
        columns = parts_of(jnp.concatenate([tops[...], bottoms[...]], axis=1))
        between[half] = product_of(parts_of(arrived_block[...]), columns, FIRST)
        for n, d in enumerate(RING):
            send(between.at[half, ring_place(d)], shares_c.at[half, n], cross_send, cross_recv.at[half], ring_row(d), col)

    pl.delay(1)
    cross_products(0)

    pl.delay(1)
    here = ring_place(0)
    await_bytes(shares_tt, sum_recv.at[0])
    mine = partial[0, here]
    for n in range(ring):
        mine = mine + shares_tt[n]
    total_mine[0] = mine
    total[0, here] = mine
    for d in RING:
        send(total_mine.at[0], total.at[0, here], all_send, all_recv.at[0], ring_row(d), col)
    await_bytes(shares_b, sum_recv.at[1])
    mine = partial[1:3, here]
    for n in range(ring):
        mine = mine + shares_b[n]
    total_mine[1:3] = mine
    total[1:3, here] = mine
    for d in RING:
        send(total_mine.at[1:3], total.at[1:3, here], all_send, all_recv.at[1], ring_row(d), col)
    pl.delay(1)
    cross_products(1)
    pl.delay(1)
    await_bytes(total.at[0, : ring * share], all_recv.at[0])
    await_bytes(total.at[1:3, : ring * share], all_recv.at[1])

    pl.delay(1)
    cross = total[1]
    gram = jnp.concatenate(
        [jnp.concatenate([total[0], jnp.transpose(cross)], axis=1), jnp.concatenate([cross, total[2]], axis=1)], axis=0
    )
    rounds = plan_ref.shape[1]

    def first_plan(r):
        return plan_ref[0, r : r + 1, :]

    def tell(r, cosine, sine):
        turns_out[r] = jnp.concatenate([cosine, sine], axis=0)
        send(turns_out.at[r], turns_in.at[r], next_send, next_recv.at[2 + r], rows, after)

    rotation, image = solve(gram, first_plan, rounds, tell)
    pl.delay(1)
    await_bytes(shares_c.at[0], cross_recv.at[0])
    await_bytes(shares_c.at[1], cross_recv.at[1])
    pl.delay(1)
    mine = between[:, here]
    for n in range(ring):
        mine = mine + shares_c[:, n]
    turn = parts_of(rotation)
    left = [part[:, :BLOCK] for part in turn]
    mine = product_of(parts_of(mine.reshape(2 * share, WIDTH)), left).reshape(2, share, BLOCK)
    half_turned_mine[...] = mine
    half_turned[:, here] = mine
    for d in RING:
        send(half_turned_mine, half_turned.at[:, here], all2_send, all2_recv, ring_row(d), col)
    pl.delay(1)
    square_out[...] = full_product(rotation[:, BLOCK:], image[:, BLOCK:], FIRST)
    top_square = full_product(rotation[:, :BLOCK], image[:, :BLOCK], FIRST)
    send(square_out, square_in, next_send, next_recv.at[2 + rounds], rows, after)

    pl.delay(1)
    columns = parts_of(jnp.concatenate([tops[...], bottoms[...]], axis=1))
    tops_now[...] = product_of(columns, left)
    next_rotation = None
    for r in range(rounds):
        await_bytes(turns_in.at[r], next_recv.at[2 + r])
        next_rotation = turned_by(next_rotation, first_plan(r), turns_in[r, 0:1, :], turns_in[r, 1:2, :])
    right = [part[:, BLOCK:] for part in parts_of(next_rotation)]
    next_columns = parts_of(jnp.concatenate([next_tops[...], next_bottoms[...]], axis=1))
    bottoms_in[...] = product_of(next_columns, right)
    pl.delay(1)
    await_bytes(square_in, next_recv.at[2 + rounds])
    await_bytes(half_turned.at[:, : ring * share], all2_recv)
    pl.delay(1)
    cross = product_of(parts_of(half_turned[...].reshape(WIDTH, BLOCK)), right, FIRST)
    gram = jnp.concatenate(
        [jnp.concatenate([top_square, cross], axis=1), jnp.concatenate([jnp.transpose(cross), square_in[...]], axis=1)],
        axis=0,
    )
    rotation, _ = solve(gram, lambda r: plan_ref[1, r : r + 1, :], rounds, lambda *_: None)

    pl.delay(1)
    turn = parts_of(rotation)
    for k, (a, b) in enumerate(PEERS + ((0, 0),)):
     if True:
        place = pl.ds(pl.multiple_of(member(a, b) * chunk, chunk), chunk)
        now = product_of(parts_of(jnp.concatenate([tops_now[place], bottoms_in[place]], axis=1)), turn)
        result_out[k, 1] = now[:, BLOCK:]
        send(result_out.at[k, 1], result.at[2 * me + 1], out_send, out_recv, row_of(a, b), after)
        if k < near:
            result_out[k, 0] = now[:, :BLOCK]
            send(result_out.at[k, 0], result.at[2 * me], out_send, out_recv, row_of(a, b), col)
        else:
            result[2 * me] = now[:, :BLOCK]
    pl.delay(1)
    await_bytes(result.at[: 2 * near + 1], out_recv)
    pl.delay(1)
    await_bytes(x_own.at[: 2 * near], in_send)
    await_bytes(tops.at[: 3 * ring * share], sum_send)
    await_bytes(tops.at[: 3 * ring * share], all_send)
    await_bytes(tops, next_send)
    await_bytes(bottoms, next_send)
    await_bytes(turns_out, next_send)
    await_bytes(square_out, next_send)
    await_bytes(shares_c, cross_send)
    await_bytes(half_turned.at[:, : ring * share], all2_send)
    await_bytes(result.at[: 2 * near + 1], out_send)


def body(matrix, plan):
    chunk, pairs, halves, width = matrix.shape
    slots = pairs * halves
    every = chunk * GROUP
    share = BLOCK // ZS
    f32 = jnp.float32
    dma = pltpu.SemaphoreType.DMA
    near, ring = len(PEERS), len(RING)
    vmem = pltpu.VMEM
    result = pl.pallas_call(
        kernel,
        out_shape=jax.ShapeDtypeStruct((slots, chunk, width), f32),
        in_specs=[pl.BlockSpec(memory_space=pltpu.HBM)] * 2,
        out_specs=pl.BlockSpec(memory_space=pltpu.VMEM),
        scratch_shapes=[
            vmem(plan.shape, jnp.int32),
            vmem((slots, chunk, width), f32),
            vmem((every, width), f32),
            vmem((every, width), f32),
            vmem((3, BLOCK, BLOCK), f32),
            vmem((ring, share, BLOCK), f32),
            vmem((ring, 2, share, BLOCK), f32),
            vmem((3, BLOCK, BLOCK), f32),
            vmem((3, share, BLOCK), f32),
            vmem((every, width), f32),
            vmem((every, width), f32),
            vmem((plan.shape[1], 2, WIDTH), f32),
            vmem((plan.shape[1], 2, WIDTH), f32),
            vmem((every, width), f32),
            vmem((BLOCK, BLOCK), f32),
            vmem((BLOCK, BLOCK), f32),
            vmem((every, width), f32),
            vmem((2, BLOCK, WIDTH), f32),
            vmem((2, ring, share, WIDTH), f32),
            vmem((2, BLOCK, BLOCK), f32),
            vmem((2, share, BLOCK), f32),
            vmem((near + 1, 2, chunk, width), f32),
            dma((3,)),
            dma,
            dma((2, 2)),
            dma,
            dma((2,)),
            dma,
            dma((2,)),
            dma,
            dma((7,)),
            dma,
            dma((2,)),
            dma,
            dma,
            dma,
            dma,
        ],
        compiler_params=pltpu.CompilerParams(collective_id=0, has_side_effects=True, vmem_limit_bytes=24 * 2**20),
        cost_estimate=pl.CostEstimate(flops=10**9, bytes_accessed=2 * matrix.size * 4, transcendentals=0),
        name="jacobi_steps",
    )(pltpu.with_memory_space_constraint(matrix.reshape(chunk, slots, width), pltpu.HBM), pltpu.with_memory_space_constraint(plan, pltpu.HBM))
    return result.transpose(1, 0, 2).reshape(matrix.shape)


def solution(mesh):
    in_specs = (P("rows", "cols", None, None), P())
    out_specs = P("rows", "cols", None, None)
    return jax.shard_map(body, mesh=mesh, in_specs=in_specs, out_specs=out_specs, check_vma=False)
```

```python
import functools

import jax
import jax.numpy as jnp
from jax import lax
from jax.experimental import pallas as pl
from jax.experimental.pallas import tpu as pltpu
from jax.sharding import PartitionSpec as P

MESH = pl.DeviceIdType.MESH
XS, ZS, YS, CS = 4, 8, 2, 4
GROUP = XS * YS
BLOCK = 128
WIDTH = 2 * BLOCK
PEERS = ((2, 1), (0, 1), (1, 1), (2, 0), (3, 1), (1, 0), (3, 0))
RING = (4, 3, 5, 2, 6, 1, 7)
FIRST = (((0,), (0,)), ((), ()))
PLAIN = (((1,), (0,)), ((), ()))


def parts_of(value):
    high = value.astype(jnp.bfloat16)
    rest = value - high.astype(jnp.float32)
    middle = rest.astype(jnp.bfloat16)
    low = (rest - middle.astype(jnp.float32)).astype(jnp.bfloat16)
    return high, middle, low


def product(a, b, dims):
    return lax.dot_general(a, b, dims, preferred_element_type=jnp.float32)


def full_product(a, b, dims=PLAIN):
    return lax.dot_general(
        a, b, dims, precision=lax.Precision.HIGHEST, preferred_element_type=jnp.float32
    )


def product_of(a, b, dims=PLAIN):
    high = product(a[0], b[0], dims)
    return high + (product(a[0], b[1], dims) + product(a[1], b[0], dims))


def times_onehot(value, partner):
    rows = lax.broadcasted_iota(jnp.int32, (WIDTH, WIDTH), 0)
    onehot = (rows == partner).astype(jnp.float32).astype(jnp.bfloat16)
    high, middle, low = parts_of(value)
    return product(high, onehot, PLAIN) + (product(middle, onehot, PLAIN) + product(low, onehot, PLAIN))


def columns_moved(value, partner):
    rows = value.shape[0]
    near = jnp.where(partner < BLOCK, partner, partner - BLOCK)
    sides = []
    for half in range(2):
        lanes = slice(half * BLOCK, (half + 1) * BLOCK)
        index = jnp.broadcast_to(near[:, lanes], (rows, BLOCK))
        left = jnp.broadcast_to(partner[:, lanes] < BLOCK, (rows, BLOCK))
        picked = [
            jnp.take_along_axis(value[:, n * BLOCK : (n + 1) * BLOCK], index, axis=1, mode="promise_in_bounds")
            for n in range(2)
        ]
        sides.append(jnp.where(left, picked[0], picked[1]))
    return jnp.concatenate(sides, axis=1)


def solve(gram, plan_of_round, rounds, tell):
    below = lax.broadcasted_iota(jnp.int32, (WIDTH, WIDTH), 0)
    along = lax.broadcasted_iota(jnp.int32, (WIDTH, WIDTH), 1)
    index = lax.broadcasted_iota(jnp.int32, (1, WIDTH), 1)
    rotation = None
    image = gram
    for r in range(rounds):
        partner = plan_of_round(r)
        if r == 0:
            unit = below == along
            pairing = below == partner
            own = jnp.sum(jnp.where(unit, gram, 0.0), axis=0, keepdims=True)
            cross = jnp.sum(jnp.where(pairing, gram, 0.0), axis=0, keepdims=True)
        else:
            own = jnp.sum(rotation * image, axis=0, keepdims=True)
            rotation_moved = columns_moved(rotation, partner)
            cross = jnp.sum(rotation_moved * image, axis=0, keepdims=True)
        other = columns_moved(jnp.broadcast_to(own, (8, WIDTH)), partner)[:1]
        orient = jnp.where(index < partner, 1.0, -1.0)
        spread = orient * (other - own)
        sign = jnp.where(spread >= 0.0, 1.0, -1.0)
        tangent = sign * 2.0 * cross / (jnp.abs(spread) + jnp.sqrt(spread * spread + 4.0 * cross * cross))
        cosine = lax.rsqrt(1.0 + tangent * tangent)
        sine = -orient * (tangent * cosine)
        tell(r, cosine, sine)
        if r == 0:
            rotation = jnp.where(unit, cosine, 0.0) + jnp.where(pairing, sine, 0.0)
        else:
            rotation = rotation * cosine + rotation_moved * sine
        image = image * cosine + columns_moved(image, partner) * sine
    return rotation, image


def kernel(
    x_hbm,
    plan_hbm,
    result,
    plan_ref,
    x_own,
    tops,
    bottoms,
    partial,
    shares_tt,
    shares_b,
    total,
    total_mine,
    next_tops,
    next_bottoms,
    turns_out,
    turns_in,
    bottoms_in,
    square_out,
    square_in,
    tops_now,
    between,
    shares_c,
    half_turned,
    half_turned_mine,
    result_out,
    load_sem,
    in_send,
    in_recv,
    sum_send,
    sum_recv,
    all_send,
    all_recv,
    next_send,
    next_recv,
    cross_send,
    cross_recv,
    all2_send,
    all2_recv,
    out_send,
    out_recv,
):
    rows = lax.axis_index("rows")
    col = lax.axis_index("cols")
    x = rows // (ZS * YS)
    z = (rows // YS) % ZS
    y = rows % YS
    me = x * YS + y
    chunk = x_own.shape[1]
    every = tops.shape[0]
    share = BLOCK // ZS
    near, ring = len(PEERS), len(RING)
    early = near // 2

    def member(a, b):
        return ((x + a) % XS) * YS + (y + b) % YS

    def row_of(a, b):
        return (((x + a) % XS) * ZS + z) * YS + (y + b) % YS

    def ring_row(d):
        return (x * ZS + (z + d) % ZS) * YS + y

    after = (col + 1) % CS
    before = (col + CS - 1) % CS

    def send(src, dst, send_sem, recv_sem, row, column):
        pltpu.make_async_remote_copy(
            src_ref=src, dst_ref=dst, send_sem=send_sem, recv_sem=recv_sem, device_id=(row, column), device_id_type=MESH
        ).start()

    def await_bytes(like, sem):
        pltpu.make_async_remote_copy(
            src_ref=like, dst_ref=like, send_sem=sem, recv_sem=sem, device_id=(rows, col), device_id_type=MESH
        ).wait_recv()

    barrier = pltpu.get_barrier_semaphore()

    def greet(row, column):
        pl.semaphore_signal(barrier, inc=1, device_id=(row, column), device_id_type=MESH)

    for a, b in PEERS:
        greet(row_of(a, b), col)
        greet(row_of(a, b), before)
    greet(rows, before)
    for d in RING:
        greet(ring_row(d), col)

    own_place = pl.ds(pl.multiple_of(me * chunk, chunk), chunk)
    loads = ([], [])
    for half in range(2):
        for a, b in PEERS:
            slot = 2 * member(a, b) + half
            loads[half].append(pltpu.make_async_copy(x_hbm.at[:, slot, :], x_own.at[slot], load_sem.at[half]))
        gathered = (tops, bottoms)[half]
        loads[half].append(pltpu.make_async_copy(x_hbm.at[:, 2 * me + half, :], gathered.at[own_place], load_sem.at[half]))
        for load in loads[half]:
            load.start()
    plan_copy = pltpu.make_async_copy(plan_hbm, plan_ref, load_sem.at[2])
    plan_copy.start()

    pl.delay(1)
    pl.semaphore_wait(barrier, 2 * near + 1 + ring)

    pl.delay(1)
    for half in range(2):
        gathered = (tops, bottoms)[half]
        for load in loads[half]:
            load.wait()
        for k, (a, b) in enumerate(PEERS):
            send(
                x_own.at[2 * member(a, b) + half],
                gathered.at[own_place],
                in_send,
                in_recv.at[half, int(k >= early)],
                row_of(a, b),
                col,
            )
    plan_copy.wait()

    def ring_place(d):
        return pl.ds(pl.multiple_of(((z + d) % ZS) * share, share), share)

    pl.delay(1)
    def lines_of(gathered, batch):
        offsets = ((0, 0), *PEERS[:early]) if batch == 0 else PEERS[early:]
        places = [pl.ds(pl.multiple_of(member(XS - a, YS - b) * chunk, chunk), chunk) for a, b in offsets]
        return jnp.concatenate([gathered[place] for place in places], axis=0)

    def arrived(gathered, half, batch):
        count = near - early if batch else early
        await_bytes(gathered.at[: count * chunk], in_recv.at[half, batch])

    arrived(tops, 0, 0)
    tops_early = lines_of(tops, 0)
    square_early = full_product(tops_early, tops_early, FIRST)
    arrived(tops, 0, 1)
    pl.delay(1)
    @pl.when(col % 2 == 0)
    def _():
        send(tops, next_tops, next_send, next_recv.at[0], rows, after)

    tops_late = lines_of(tops, 1)
    partial[0] = square_early + full_product(tops_late, tops_late, FIRST)
    for n, d in enumerate(RING):
        send(partial.at[0, ring_place(d)], shares_tt.at[n], sum_send, sum_recv.at[0], ring_row(d), col)

    pl.delay(1)
    arrived(bottoms, 1, 0)
    bottoms_early = lines_of(bottoms, 0)
    both_early = full_product(bottoms_early, jnp.concatenate([tops_early, bottoms_early], axis=1), FIRST)
    arrived(bottoms, 1, 1)
    pl.delay(1)
    bottoms_late = lines_of(bottoms, 1)
    both = both_early + full_product(bottoms_late, jnp.concatenate([tops_late, bottoms_late], axis=1), FIRST)
    partial[1] = both[:, :BLOCK]
    partial[2] = both[:, BLOCK:]
    for n, d in enumerate(RING):
        send(partial.at[1:3, ring_place(d)], shares_b.at[n], sum_send, sum_recv.at[1], ring_row(d), col)

    @pl.when(col % 2 == 1)
    def _():
        send(tops, next_tops, next_send, next_recv.at[0], rows, after)

    send(bottoms, next_bottoms, next_send, next_recv.at[1], rows, after)

    def cross_products(half):
        arrived_block = (next_tops, next_bottoms)[half]
        await_bytes(arrived_block, next_recv.at[half])
        columns = parts_of(jnp.concatenate([tops[...], bottoms[...]], axis=1))
        between[half] = product_of(parts_of(arrived_block[...]), columns, FIRST)
        for n, d in enumerate(RING):
            send(between.at[half, ring_place(d)], shares_c.at[half, n], cross_send, cross_recv.at[half], ring_row(d), col)

    pl.delay(1)
    cross_products(0)

    pl.delay(1)
    here = ring_place(0)
    await_bytes(shares_tt, sum_recv.at[0])
    mine = partial[0, here]
    for n in range(ring):
        mine = mine + shares_tt[n]
    total_mine[0] = mine
    total[0, here] = mine
    for d in RING:
        send(total_mine.at[0], total.at[0, here], all_send, all_recv.at[0], ring_row(d), col)
    await_bytes(shares_b, sum_recv.at[1])
    mine = partial[1:3, here]
    for n in range(ring):
        mine = mine + shares_b[n]
    total_mine[1:3] = mine
    total[1:3, here] = mine
    for d in RING:
        send(total_mine.at[1:3], total.at[1:3, here], all_send, all_recv.at[1], ring_row(d), col)
    pl.delay(1)
    cross_products(1)
    pl.delay(1)
    await_bytes(total.at[0, : ring * share], all_recv.at[0])
    await_bytes(total.at[1:3, : ring * share], all_recv.at[1])

    pl.delay(1)
    cross = total[1]
    gram = jnp.concatenate(
        [jnp.concatenate([total[0], jnp.transpose(cross)], axis=1), jnp.concatenate([cross, total[2]], axis=1)], axis=0
    )
    rounds = plan_ref.shape[1]

    def first_plan(r):
        return plan_ref[0, r : r + 1, :]

    def tell(r, cosine, sine):
        turns_out[r] = jnp.concatenate([cosine, sine], axis=0)
        send(turns_out.at[r], turns_in.at[r], next_send, next_recv.at[2 + r], rows, after)

    rotation, image = solve(gram, first_plan, rounds, tell)
    pl.delay(1)
    await_bytes(shares_c.at[0], cross_recv.at[0])
    await_bytes(shares_c.at[1], cross_recv.at[1])
    pl.delay(1)
    mine = between[:, here]
    for n in range(ring):
        mine = mine + shares_c[:, n]
    turn = parts_of(rotation)
    left = [part[:, :BLOCK] for part in turn]
    mine = product_of(parts_of(mine.reshape(2 * share, WIDTH)), left).reshape(2, share, BLOCK)
    half_turned_mine[...] = mine
    half_turned[:, here] = mine
    for d in RING:
        send(half_turned_mine, half_turned.at[:, here], all2_send, all2_recv, ring_row(d), col)
    pl.delay(1)
    square_out[...] = full_product(rotation[:, BLOCK:], image[:, BLOCK:], FIRST)
    top_square = full_product(rotation[:, :BLOCK], image[:, :BLOCK], FIRST)
    send(square_out, square_in, next_send, next_recv.at[2 + rounds], rows, after)

    pl.delay(1)
    below = lax.broadcasted_iota(jnp.int32, (WIDTH, WIDTH), 0)
    along = lax.broadcasted_iota(jnp.int32, (WIDTH, WIDTH), 1)
    next_rotation = None
    for r in range(rounds):
        moved = times_onehot(next_rotation, first_plan(r)) if r else None
        await_bytes(turns_in.at[r], next_recv.at[2 + r])
        cosine, sine = turns_in[r, 0:1, :], turns_in[r, 1:2, :]
        if r:
            next_rotation = next_rotation * cosine + moved * sine
        else:
            next_rotation = jnp.where(below == along, cosine, 0.0) + jnp.where(below == first_plan(r), sine, 0.0)
    right = [part[:, BLOCK:] for part in parts_of(next_rotation)]
    pl.delay(1)
    await_bytes(square_in, next_recv.at[2 + rounds])
    await_bytes(half_turned.at[:, : ring * share], all2_recv)
    pl.delay(1)
    cross = product_of(parts_of(half_turned[...].reshape(WIDTH, BLOCK)), right, FIRST)
    gram = jnp.concatenate(
        [jnp.concatenate([top_square, cross], axis=1), jnp.concatenate([jnp.transpose(cross), square_in[...]], axis=1)],
        axis=0,
    )
    columns = parts_of(jnp.concatenate([tops[...], bottoms[...]], axis=1))
    tops_now[...] = product_of(columns, left)
    next_columns = parts_of(jnp.concatenate([next_tops[...], next_bottoms[...]], axis=1))
    bottoms_in[...] = product_of(next_columns, right)
    rotation, _ = solve(gram, lambda r: plan_ref[1, r : r + 1, :], rounds, lambda *_: None)

    pl.delay(1)
    turn = parts_of(rotation)
    targets = PEERS + ((0, 0),)
    for first, last in ((0, 1), (1, 4), (4, 8)):
        places = [pl.ds(pl.multiple_of(member(a, b) * chunk, chunk), chunk) for a, b in targets[first:last]]
        lines = [jnp.concatenate([tops_now[place], bottoms_in[place]], axis=1) for place in places]
        now = product_of(parts_of(jnp.concatenate(lines, axis=0)), turn)
        for k in range(first, last):
            part = now[(k - first) * chunk : (k - first + 1) * chunk]
            result_out[k, 1] = part[:, BLOCK:]
            if k < near:
                result_out[k, 0] = part[:, :BLOCK]
            else:
                result[2 * me] = part[:, :BLOCK]
        for k in range(first, last):
            row = row_of(*targets[k])
            send(result_out.at[k, 1], result.at[2 * me + 1], out_send, out_recv, row, after)
            if k < near:
                send(result_out.at[k, 0], result.at[2 * me], out_send, out_recv, row, col)
    pl.delay(1)
    await_bytes(result.at[: 2 * near + 1], out_recv)
    pl.delay(1)
    await_bytes(x_own.at[: 2 * near], in_send)
    await_bytes(tops.at[: 3 * ring * share], sum_send)
    await_bytes(tops.at[: 3 * ring * share], all_send)
    await_bytes(tops, next_send)
    await_bytes(bottoms, next_send)
    await_bytes(turns_out, next_send)
    await_bytes(square_out, next_send)
    await_bytes(shares_c, cross_send)
    await_bytes(half_turned.at[:, : ring * share], all2_send)
    await_bytes(result.at[: 2 * near + 1], out_send)


def place_kernel(result, out, sem):
    copies = [pltpu.make_async_copy(result.at[n], out.at[:, n, :], sem) for n in range(result.shape[0])]
    for copy in copies:
        copy.start()
    for copy in copies:
        copy.wait()


def body(matrix, plan):
    chunk, pairs, halves, width = matrix.shape
    slots = pairs * halves
    every = chunk * GROUP
    share = BLOCK // ZS
    f32 = jnp.float32
    dma = pltpu.SemaphoreType.DMA
    near, ring = len(PEERS), len(RING)
    vmem = pltpu.VMEM
    result = pl.pallas_call(
        kernel,
        out_shape=jax.ShapeDtypeStruct((slots, chunk, width), f32),
        in_specs=[pl.BlockSpec(memory_space=pltpu.HBM)] * 2,
        out_specs=pl.BlockSpec(memory_space=pltpu.VMEM),
        scratch_shapes=[
            vmem(plan.shape, jnp.int32),
            vmem((slots, chunk, width), f32),
            vmem((every, width), f32),
            vmem((every, width), f32),
            vmem((3, BLOCK, BLOCK), f32),
            vmem((ring, share, BLOCK), f32),
            vmem((ring, 2, share, BLOCK), f32),
            vmem((3, BLOCK, BLOCK), f32),
            vmem((3, share, BLOCK), f32),
            vmem((every, width), f32),
            vmem((every, width), f32),
            vmem((plan.shape[1], 2, WIDTH), f32),
            vmem((plan.shape[1], 2, WIDTH), f32),
            vmem((every, width), f32),
            vmem((BLOCK, BLOCK), f32),
            vmem((BLOCK, BLOCK), f32),
            vmem((every, width), f32),
            vmem((2, BLOCK, WIDTH), f32),
            vmem((2, ring, share, WIDTH), f32),
            vmem((2, BLOCK, BLOCK), f32),
            vmem((2, share, BLOCK), f32),
            vmem((near + 1, 2, chunk, width), f32),
            dma((3,)),
            dma,
            dma((2, 2)),
            dma,
            dma((2,)),
            dma,
            dma((2,)),
            dma,
            dma((7,)),
            dma,
            dma((2,)),
            dma,
            dma,
            dma,
            dma,
        ],
        compiler_params=pltpu.CompilerParams(collective_id=0, has_side_effects=True, vmem_limit_bytes=24 * 2**20),
        cost_estimate=pl.CostEstimate(flops=10**9, bytes_accessed=2 * matrix.size * 4, transcendentals=0),
        name="jacobi_steps",
    )(pltpu.with_memory_space_constraint(matrix.reshape(chunk, slots, width), pltpu.HBM), pltpu.with_memory_space_constraint(plan, pltpu.HBM))
    placed = pl.pallas_call(
        place_kernel,
        out_shape=jax.ShapeDtypeStruct((chunk, slots, width), f32),
        in_specs=[pl.BlockSpec(memory_space=pltpu.VMEM)],
        out_specs=pl.BlockSpec(memory_space=pltpu.HBM),
        scratch_shapes=[dma],
        compiler_params=pltpu.CompilerParams(vmem_limit_bytes=2**20),
        name="place",
    )(result)
    return placed.reshape(matrix.shape)


def solution(mesh):
    in_specs = (P("rows", "cols", None, None), P())
    out_specs = P("rows", "cols", None, None)
    return jax.shard_map(body, mesh=mesh, in_specs=in_specs, out_specs=out_specs, check_vma=False)
```

```python
import functools

import jax
import jax.numpy as jnp
from jax import lax
from jax.experimental import pallas as pl
from jax.experimental.pallas import tpu as pltpu
from jax.sharding import PartitionSpec as P

MESH = pl.DeviceIdType.MESH
XS, ZS, YS, CS = 4, 8, 2, 4
GROUP = XS * YS
BLOCK = 128
WIDTH = 2 * BLOCK
PEERS = ((2, 1), (0, 1), (1, 1), (2, 0), (3, 1), (1, 0), (3, 0))
RING = (4, 3, 5, 2, 6, 1, 7)
FIRST = (((0,), (0,)), ((), ()))
PLAIN = (((1,), (0,)), ((), ()))


def parts_of(value):
    high = value.astype(jnp.bfloat16)
    rest = value - high.astype(jnp.float32)
    middle = rest.astype(jnp.bfloat16)
    low = (rest - middle.astype(jnp.float32)).astype(jnp.bfloat16)
    return high, middle, low


def product(a, b, dims):
    return lax.dot_general(a, b, dims, preferred_element_type=jnp.float32)


def full_product(a, b, dims=PLAIN):
    return lax.dot_general(
        a, b, dims, precision=lax.Precision.HIGHEST, preferred_element_type=jnp.float32
    )


def product_of(a, b, dims=PLAIN):
    high = product(a[0], b[0], dims)
    return high + (product(a[0], b[1], dims) + product(a[1], b[0], dims))


def times_onehot(value, partner):
    rows = lax.broadcasted_iota(jnp.int32, (WIDTH, WIDTH), 0)
    onehot = (rows == partner).astype(jnp.float32).astype(jnp.bfloat16)
    high, middle, low = parts_of(value)
    return product(high, onehot, PLAIN) + (product(middle, onehot, PLAIN) + product(low, onehot, PLAIN))


def columns_moved(value, partner):
    rows = value.shape[0]
    near = jnp.where(partner < BLOCK, partner, partner - BLOCK)
    sides = []
    for half in range(2):
        lanes = slice(half * BLOCK, (half + 1) * BLOCK)
        index = jnp.broadcast_to(near[:, lanes], (rows, BLOCK))
        left = jnp.broadcast_to(partner[:, lanes] < BLOCK, (rows, BLOCK))
        picked = [
            jnp.take_along_axis(value[:, n * BLOCK : (n + 1) * BLOCK], index, axis=1, mode="promise_in_bounds")
            for n in range(2)
        ]
        sides.append(jnp.where(left, picked[0], picked[1]))
    return jnp.concatenate(sides, axis=1)


def solve(gram, plan_of_round, rounds, tell):
    below = lax.broadcasted_iota(jnp.int32, (WIDTH, WIDTH), 0)
    along = lax.broadcasted_iota(jnp.int32, (WIDTH, WIDTH), 1)
    index = lax.broadcasted_iota(jnp.int32, (1, WIDTH), 1)
    rotation = None
    image = gram
    for r in range(rounds):
        partner = plan_of_round(r)
        if r == 0:
            unit = below == along
            pairing = below == partner
            own = jnp.sum(jnp.where(unit, gram, 0.0), axis=0, keepdims=True)
            cross = jnp.sum(jnp.where(pairing, gram, 0.0), axis=0, keepdims=True)
        else:
            own = jnp.sum(rotation * image, axis=0, keepdims=True)
            rotation_moved = columns_moved(rotation, partner)
            cross = jnp.sum(rotation_moved * image, axis=0, keepdims=True)
        other = columns_moved(jnp.broadcast_to(own, (8, WIDTH)), partner)[:1]
        orient = jnp.where(index < partner, 1.0, -1.0)
        spread = orient * (other - own)
        sign = jnp.where(spread >= 0.0, 1.0, -1.0)
        tangent = sign * 2.0 * cross / (jnp.abs(spread) + jnp.sqrt(spread * spread + 4.0 * cross * cross))
        cosine = lax.rsqrt(1.0 + tangent * tangent)
        sine = -orient * (tangent * cosine)
        tell(r, cosine, sine)
        if r == 0:
            rotation = jnp.where(unit, cosine, 0.0) + jnp.where(pairing, sine, 0.0)
        else:
            rotation = rotation * cosine + rotation_moved * sine
        image = image * cosine + columns_moved(image, partner) * sine
    return rotation, image


def kernel(
    x_hbm,
    plan_hbm,
    result,
    plan_ref,
    x_own,
    tops,
    bottoms,
    partial,
    shares_tt,
    shares_b,
    total,
    total_mine,
    diagonals,
    diagonal_mine,
    next_tops,
    next_bottoms,
    turns_out,
    turns_in,
    bottoms_in,
    square_out,
    square_in,
    tops_now,
    between,
    shares_c,
    half_turned,
    half_turned_mine,
    result_out,
    load_sem,
    in_send,
    in_recv,
    sum_send,
    sum_recv,
    all_send,
    all_recv,
    next_send,
    next_recv,
    cross_send,
    cross_recv,
    all2_send,
    all2_recv,
    out_send,
    out_recv,
):
    rows = lax.axis_index("rows")
    col = lax.axis_index("cols")
    x = rows // (ZS * YS)
    z = (rows // YS) % ZS
    y = rows % YS
    me = x * YS + y
    chunk = x_own.shape[1]
    every = tops.shape[0]
    share = BLOCK // ZS
    near, ring = len(PEERS), len(RING)
    early = near // 2

    def member(a, b):
        return ((x + a) % XS) * YS + (y + b) % YS

    def row_of(a, b):
        return (((x + a) % XS) * ZS + z) * YS + (y + b) % YS

    def ring_row(d):
        return (x * ZS + (z + d) % ZS) * YS + y

    after = (col + 1) % CS
    before = (col + CS - 1) % CS

    def send(src, dst, send_sem, recv_sem, row, column):
        pltpu.make_async_remote_copy(
            src_ref=src, dst_ref=dst, send_sem=send_sem, recv_sem=recv_sem, device_id=(row, column), device_id_type=MESH
        ).start()

    def await_bytes(like, sem):
        pltpu.make_async_remote_copy(
            src_ref=like, dst_ref=like, send_sem=sem, recv_sem=sem, device_id=(rows, col), device_id_type=MESH
        ).wait_recv()

    barrier = pltpu.get_barrier_semaphore()

    def greet(row, column):
        pl.semaphore_signal(barrier, inc=1, device_id=(row, column), device_id_type=MESH)

    for a, b in PEERS:
        greet(row_of(a, b), col)
        greet(row_of(a, b), before)
    greet(rows, before)
    for d in RING:
        greet(ring_row(d), col)

    own_place = pl.ds(pl.multiple_of(me * chunk, chunk), chunk)
    loads = ([], [])
    for half in range(2):
        for a, b in PEERS:
            slot = 2 * member(a, b) + half
            loads[half].append(pltpu.make_async_copy(x_hbm.at[:, slot, :], x_own.at[slot], load_sem.at[half]))
        gathered = (tops, bottoms)[half]
        loads[half].append(pltpu.make_async_copy(x_hbm.at[:, 2 * me + half, :], gathered.at[own_place], load_sem.at[half]))
        for load in loads[half]:
            load.start()
    plan_copy = pltpu.make_async_copy(plan_hbm, plan_ref, load_sem.at[2])
    plan_copy.start()

    pl.delay(1)
    pl.semaphore_wait(barrier, 2 * near + 1 + ring)

    pl.delay(1)
    for half in range(2):
        gathered = (tops, bottoms)[half]
        for load in loads[half]:
            load.wait()
        for k, (a, b) in enumerate(PEERS):
            send(
                x_own.at[2 * member(a, b) + half],
                gathered.at[own_place],
                in_send,
                in_recv.at[half, int(k >= early)],
                row_of(a, b),
                col,
            )
    plan_copy.wait()

    def ring_place(d):
        return pl.ds(pl.multiple_of(((z + d) % ZS) * share, share), share)

    pl.delay(1)
    def lines_of(gathered, batch):
        offsets = ((0, 0), *PEERS[:early]) if batch == 0 else PEERS[early:]
        places = [pl.ds(pl.multiple_of(member(XS - a, YS - b) * chunk, chunk), chunk) for a, b in offsets]
        return jnp.concatenate([gathered[place] for place in places], axis=0)

    def arrived(gathered, half, batch):
        count = near - early if batch else early
        await_bytes(gathered.at[: count * chunk], in_recv.at[half, batch])

    arrived(tops, 0, 0)
    tops_early = lines_of(tops, 0)
    square_early = full_product(tops_early, tops_early, FIRST)
    arrived(tops, 0, 1)
    pl.delay(1)
    @pl.when(col % 2 == 0)
    def _():
        send(tops, next_tops, next_send, next_recv.at[0], rows, after)

    tops_late = lines_of(tops, 1)
    partial[0] = square_early + full_product(tops_late, tops_late, FIRST)
    for n, d in enumerate(RING):
        send(partial.at[0, ring_place(d)], shares_tt.at[n], sum_send, sum_recv.at[0], ring_row(d), col)

    pl.delay(1)
    arrived(bottoms, 1, 0)
    bottoms_early = lines_of(bottoms, 0)
    both_early = full_product(bottoms_early, jnp.concatenate([tops_early, bottoms_early], axis=1), FIRST)
    arrived(bottoms, 1, 1)
    pl.delay(1)
    bottoms_late = lines_of(bottoms, 1)
    both = both_early + full_product(bottoms_late, jnp.concatenate([tops_late, bottoms_late], axis=1), FIRST)
    partial[1] = both[:, :BLOCK]
    partial[2] = both[:, BLOCK:]
    for n, d in enumerate(RING):
        send(partial.at[1:3, ring_place(d)], shares_b.at[n], sum_send, sum_recv.at[1], ring_row(d), col)

    @pl.when(col % 2 == 1)
    def _():
        send(tops, next_tops, next_send, next_recv.at[0], rows, after)

    send(bottoms, next_bottoms, next_send, next_recv.at[1], rows, after)

    def cross_products(half):
        arrived_block = (next_tops, next_bottoms)[half]
        await_bytes(arrived_block, next_recv.at[half])
        columns = parts_of(jnp.concatenate([tops[...], bottoms[...]], axis=1))
        between[half] = product_of(parts_of(arrived_block[...]), columns, FIRST)
        for n, d in enumerate(RING):
            send(between.at[half, ring_place(d)], shares_c.at[half, n], cross_send, cross_recv.at[half], ring_row(d), col)

    pl.delay(1)
    cross_products(0)

    pl.delay(1)
    here = ring_place(0)
    await_bytes(shares_tt, sum_recv.at[0])
    own_tt = partial[0, here]
    for n in range(ring):
        own_tt = own_tt + shares_tt[n]
    await_bytes(shares_b, sum_recv.at[1])
    own_b = partial[1:3, here]
    for n in range(ring):
        own_b = own_b + shares_b[n]
    line = lax.broadcasted_iota(jnp.int32, (share, BLOCK), 0) + z * share
    lane = lax.broadcasted_iota(jnp.int32, (share, BLOCK), 1)
    mine = jnp.stack([own_b[0], jnp.where(lane >= line, own_tt, own_b[1])], axis=0)
    total_mine[...] = mine
    total[:, here] = mine
    diagonal = jnp.sum(jnp.where(lane == line, own_b[1], 0.0), axis=0, keepdims=True)
    diagonal_mine[...] = diagonal
    diagonals[z] = diagonal
    for d in RING:
        send(total_mine, total.at[:, here], all_send, all_recv.at[0], ring_row(d), col)
        send(diagonal_mine, diagonals.at[z], all_send, all_recv.at[1], ring_row(d), col)
    pl.delay(1)
    cross_products(1)
    pl.delay(1)
    await_bytes(total.at[:, : ring * share], all_recv.at[0])
    await_bytes(diagonals.at[:ring], all_recv.at[1])

    pl.delay(1)
    cross = total[0]
    packed = total[1]
    flipped = jnp.transpose(packed)
    line = lax.broadcasted_iota(jnp.int32, (BLOCK, BLOCK), 0)
    lane = lax.broadcasted_iota(jnp.int32, (BLOCK, BLOCK), 1)
    diagonal = jnp.sum(diagonals[...], axis=0)
    top_gram = jnp.where(lane >= line, packed, flipped)
    bottom_gram = jnp.where(lane == line, diagonal, jnp.where(lane < line, packed, flipped))
    gram = jnp.concatenate(
        [
            jnp.concatenate([top_gram, jnp.transpose(cross)], axis=1),
            jnp.concatenate([cross, bottom_gram], axis=1),
        ],
        axis=0,
    )
    rounds = plan_ref.shape[1]

    def first_plan(r):
        return plan_ref[0, r : r + 1, :]

    def tell(r, cosine, sine):
        turns_out[r] = jnp.concatenate([cosine, sine], axis=0)
        send(turns_out.at[r], turns_in.at[r], next_send, next_recv.at[2 + r], rows, after)

    rotation, image = solve(gram, first_plan, rounds, tell)
    pl.delay(1)
    await_bytes(shares_c.at[0], cross_recv.at[0])
    await_bytes(shares_c.at[1], cross_recv.at[1])
    pl.delay(1)
    mine = between[:, here]
    for n in range(ring):
        mine = mine + shares_c[:, n]
    turn = parts_of(rotation)
    left = [part[:, :BLOCK] for part in turn]
    mine = product_of(parts_of(mine.reshape(2 * share, WIDTH)), left).reshape(2, share, BLOCK)
    half_turned_mine[...] = mine
    half_turned[:, here] = mine
    for d in RING:
        send(half_turned_mine, half_turned.at[:, here], all2_send, all2_recv, ring_row(d), col)
    pl.delay(1)
    square_out[...] = full_product(rotation[:, BLOCK:], image[:, BLOCK:], FIRST)
    top_square = full_product(rotation[:, :BLOCK], image[:, :BLOCK], FIRST)
    send(square_out, square_in, next_send, next_recv.at[2 + rounds], rows, after)

    pl.delay(1)
    below = lax.broadcasted_iota(jnp.int32, (WIDTH, WIDTH), 0)
    along = lax.broadcasted_iota(jnp.int32, (WIDTH, WIDTH), 1)
    next_rotation = None
    for r in range(rounds):
        moved = times_onehot(next_rotation, first_plan(r)) if r else None
        await_bytes(turns_in.at[r], next_recv.at[2 + r])
        cosine, sine = turns_in[r, 0:1, :], turns_in[r, 1:2, :]
        if r:
            next_rotation = next_rotation * cosine + moved * sine
        else:
            next_rotation = jnp.where(below == along, cosine, 0.0) + jnp.where(below == first_plan(r), sine, 0.0)
    right = [part[:, BLOCK:] for part in parts_of(next_rotation)]
    pl.delay(1)
    await_bytes(square_in, next_recv.at[2 + rounds])
    await_bytes(half_turned.at[:, : ring * share], all2_recv)
    pl.delay(1)
    cross = product_of(parts_of(half_turned[...].reshape(WIDTH, BLOCK)), right, FIRST)
    gram = jnp.concatenate(
        [jnp.concatenate([top_square, cross], axis=1), jnp.concatenate([jnp.transpose(cross), square_in[...]], axis=1)],
        axis=0,
    )
    columns = parts_of(jnp.concatenate([tops[...], bottoms[...]], axis=1))
    tops_now[...] = product_of(columns, left)
    next_columns = parts_of(jnp.concatenate([next_tops[...], next_bottoms[...]], axis=1))
    bottoms_in[...] = product_of(next_columns, right)
    rotation, _ = solve(gram, lambda r: plan_ref[1, r : r + 1, :], rounds, lambda *_: None)

    pl.delay(1)
    turn = parts_of(rotation)
    targets = PEERS + ((0, 0),)
    for first, last in ((0, 1), (1, 4), (4, 8)):
        places = [pl.ds(pl.multiple_of(member(a, b) * chunk, chunk), chunk) for a, b in targets[first:last]]
        lines = [jnp.concatenate([tops_now[place], bottoms_in[place]], axis=1) for place in places]
        now = product_of(parts_of(jnp.concatenate(lines, axis=0)), turn)
        for k in range(first, last):
            part = now[(k - first) * chunk : (k - first + 1) * chunk]
            result_out[k, 1] = part[:, BLOCK:]
            if k < near:
                result_out[k, 0] = part[:, :BLOCK]
            else:
                result[2 * me] = part[:, :BLOCK]
        for k in range(first, last):
            row = row_of(*targets[k])
            send(result_out.at[k, 1], result.at[2 * me + 1], out_send, out_recv, row, after)
            if k < near:
                send(result_out.at[k, 0], result.at[2 * me], out_send, out_recv, row, col)
    pl.delay(1)
    await_bytes(result.at[: 2 * near + 1], out_recv)
    pl.delay(1)
    await_bytes(x_own.at[: 2 * near], in_send)
    await_bytes(tops.at[: 3 * ring * share], sum_send)
    await_bytes(tops.at[: 2 * ring * share], all_send)
    await_bytes(diagonals.at[:ring], all_send)
    await_bytes(tops, next_send)
    await_bytes(bottoms, next_send)
    await_bytes(turns_out, next_send)
    await_bytes(square_out, next_send)
    await_bytes(shares_c, cross_send)
    await_bytes(half_turned.at[:, : ring * share], all2_send)
    await_bytes(result.at[: 2 * near + 1], out_send)


def place_kernel(result, out, sem):
    copies = [pltpu.make_async_copy(result.at[n], out.at[:, n, :], sem) for n in range(result.shape[0])]
    for copy in copies:
        copy.start()
    for copy in copies:
        copy.wait()


def body(matrix, plan):
    chunk, pairs, halves, width = matrix.shape
    slots = pairs * halves
    every = chunk * GROUP
    share = BLOCK // ZS
    f32 = jnp.float32
    dma = pltpu.SemaphoreType.DMA
    near, ring = len(PEERS), len(RING)
    vmem = pltpu.VMEM
    result = pl.pallas_call(
        kernel,
        out_shape=jax.ShapeDtypeStruct((slots, chunk, width), f32),
        in_specs=[pl.BlockSpec(memory_space=pltpu.HBM)] * 2,
        out_specs=pl.BlockSpec(memory_space=pltpu.VMEM),
        scratch_shapes=[
            vmem(plan.shape, jnp.int32),
            vmem((slots, chunk, width), f32),
            vmem((every, width), f32),
            vmem((every, width), f32),
            vmem((3, BLOCK, BLOCK), f32),
            vmem((ring, share, BLOCK), f32),
            vmem((ring, 2, share, BLOCK), f32),
            vmem((2, BLOCK, BLOCK), f32),
            vmem((2, share, BLOCK), f32),
            vmem((ZS, 1, BLOCK), f32),
            vmem((1, BLOCK), f32),
            vmem((every, width), f32),
            vmem((every, width), f32),
            vmem((plan.shape[1], 2, WIDTH), f32),
            vmem((plan.shape[1], 2, WIDTH), f32),
            vmem((every, width), f32),
            vmem((BLOCK, BLOCK), f32),
            vmem((BLOCK, BLOCK), f32),
            vmem((every, width), f32),
            vmem((2, BLOCK, WIDTH), f32),
            vmem((2, ring, share, WIDTH), f32),
            vmem((2, BLOCK, BLOCK), f32),
            vmem((2, share, BLOCK), f32),
            vmem((near + 1, 2, chunk, width), f32),
            dma((3,)),
            dma,
            dma((2, 2)),
            dma,
            dma((2,)),
            dma,
            dma((2,)),
            dma,
            dma((7,)),
            dma,
            dma((2,)),
            dma,
            dma,
            dma,
            dma,
        ],
        compiler_params=pltpu.CompilerParams(collective_id=0, has_side_effects=True, vmem_limit_bytes=24 * 2**20),
        cost_estimate=pl.CostEstimate(flops=10**9, bytes_accessed=2 * matrix.size * 4, transcendentals=0),
        name="jacobi_steps",
    )(pltpu.with_memory_space_constraint(matrix.reshape(chunk, slots, width), pltpu.HBM), pltpu.with_memory_space_constraint(plan, pltpu.HBM))
    placed = pl.pallas_call(
        place_kernel,
        out_shape=jax.ShapeDtypeStruct((chunk, slots, width), f32),
        in_specs=[pl.BlockSpec(memory_space=pltpu.VMEM)],
        out_specs=pl.BlockSpec(memory_space=pltpu.HBM),
        scratch_shapes=[dma],
        compiler_params=pltpu.CompilerParams(vmem_limit_bytes=2**20),
        name="place",
    )(result)
    return placed.reshape(matrix.shape)


def solution(mesh):
    in_specs = (P("rows", "cols", None, None), P())
    out_specs = P("rows", "cols", None, None)
    return jax.shard_map(body, mesh=mesh, in_specs=in_specs, out_specs=out_specs, check_vma=False)
```

```python
import functools

import jax
import jax.numpy as jnp
from jax import lax
from jax.experimental import pallas as pl
from jax.experimental.pallas import tpu as pltpu
from jax.sharding import PartitionSpec as P

MESH = pl.DeviceIdType.MESH
XS, ZS, YS, CS = 4, 8, 2, 4
GROUP = XS * YS
BLOCK = 128
WIDTH = 2 * BLOCK
PEERS = ((2, 1), (0, 1), (1, 1), (2, 0), (3, 1), (1, 0), (3, 0))
RING = (4, 3, 5, 2, 6, 1, 7)
FIRST = (((0,), (0,)), ((), ()))
PLAIN = (((1,), (0,)), ((), ()))


def parts_of(value):
    high = value.astype(jnp.bfloat16)
    rest = value - high.astype(jnp.float32)
    middle = rest.astype(jnp.bfloat16)
    low = (rest - middle.astype(jnp.float32)).astype(jnp.bfloat16)
    return high, middle, low


def product(a, b, dims):
    return lax.dot_general(a, b, dims, preferred_element_type=jnp.float32)


def full_product(a, b, dims=PLAIN):
    return lax.dot_general(
        a, b, dims, precision=lax.Precision.HIGHEST, preferred_element_type=jnp.float32
    )


def product_of(a, b, dims=PLAIN):
    high = product(a[0], b[0], dims)
    return high + (product(a[0], b[1], dims) + product(a[1], b[0], dims))


def times_onehot(value, partner):
    rows = lax.broadcasted_iota(jnp.int32, (WIDTH, WIDTH), 0)
    onehot = (rows == partner).astype(jnp.float32).astype(jnp.bfloat16)
    high, middle, low = parts_of(value)
    return product(high, onehot, PLAIN) + (product(middle, onehot, PLAIN) + product(low, onehot, PLAIN))


def columns_moved(value, partner):
    rows = value.shape[0]
    near = jnp.where(partner < BLOCK, partner, partner - BLOCK)
    sides = []
    for half in range(2):
        lanes = slice(half * BLOCK, (half + 1) * BLOCK)
        index = jnp.broadcast_to(near[:, lanes], (rows, BLOCK))
        left = jnp.broadcast_to(partner[:, lanes] < BLOCK, (rows, BLOCK))
        picked = [
            jnp.take_along_axis(value[:, n * BLOCK : (n + 1) * BLOCK], index, axis=1, mode="promise_in_bounds")
            for n in range(2)
        ]
        sides.append(jnp.where(left, picked[0], picked[1]))
    return jnp.concatenate(sides, axis=1)


def solve(gram, plan_of_round, rounds, tell):
    below = lax.broadcasted_iota(jnp.int32, (WIDTH, WIDTH), 0)
    along = lax.broadcasted_iota(jnp.int32, (WIDTH, WIDTH), 1)
    index = lax.broadcasted_iota(jnp.int32, (1, WIDTH), 1)
    rotation = None
    image = gram
    for r in range(rounds):
        partner = plan_of_round(r)
        if r == 0:
            unit = below == along
            pairing = below == partner
            own = jnp.sum(jnp.where(unit, gram, 0.0), axis=0, keepdims=True)
            cross = jnp.sum(jnp.where(pairing, gram, 0.0), axis=0, keepdims=True)
        else:
            own = jnp.sum(rotation * image, axis=0, keepdims=True)
            rotation_moved = columns_moved(rotation, partner)
            cross = jnp.sum(rotation_moved * image, axis=0, keepdims=True)
        other = columns_moved(jnp.broadcast_to(own, (8, WIDTH)), partner)[:1]
        orient = jnp.where(index < partner, 1.0, -1.0)
        spread = orient * (other - own)
        sign = jnp.where(spread >= 0.0, 1.0, -1.0)
        tangent = sign * 2.0 * cross / (jnp.abs(spread) + jnp.sqrt(spread * spread + 4.0 * cross * cross))
        cosine = lax.rsqrt(1.0 + tangent * tangent)
        sine = -orient * (tangent * cosine)
        tell(r, cosine, sine)
        if r == 0:
            rotation = jnp.where(unit, cosine, 0.0) + jnp.where(pairing, sine, 0.0)
        else:
            rotation = rotation * cosine + rotation_moved * sine
        image = image * cosine + columns_moved(image, partner) * sine
    return rotation, image


def kernel(
    x_hbm,
    plan_hbm,
    result,
    plan_ref,
    x_own,
    tops,
    bottoms,
    partial,
    shares_tt,
    shares_b,
    total,
    total_mine,
    diagonals,
    diagonal_mine,
    next_tops,
    next_bottoms,
    turns_out,
    turns_in,
    bottoms_in,
    square_out,
    square_in,
    tops_now,
    between,
    shares_c,
    half_turned,
    half_turned_mine,
    result_out,
    load_sem,
    in_send,
    in_recv,
    sum_send,
    sum_recv,
    all_send,
    all_recv,
    next_send,
    next_recv,
    cross_send,
    cross_recv,
    all2_send,
    all2_recv,
    out_send,
    out_recv,
):
    rows = lax.axis_index("rows")
    col = lax.axis_index("cols")
    x = rows // (ZS * YS)
    z = (rows // YS) % ZS
    y = rows % YS
    me = x * YS + y
    chunk = x_own.shape[1]
    every = tops.shape[0]
    share = BLOCK // ZS
    near, ring = len(PEERS), len(RING)
    early = near // 2

    def member(a, b):
        return ((x + a) % XS) * YS + (y + b) % YS

    def row_of(a, b):
        return (((x + a) % XS) * ZS + z) * YS + (y + b) % YS

    def ring_row(d):
        return (x * ZS + (z + d) % ZS) * YS + y

    after = (col + 1) % CS
    before = (col + CS - 1) % CS

    def send(src, dst, send_sem, recv_sem, row, column):
        pltpu.make_async_remote_copy(
            src_ref=src, dst_ref=dst, send_sem=send_sem, recv_sem=recv_sem, device_id=(row, column), device_id_type=MESH
        ).start()

    def await_bytes(like, sem):
        pltpu.make_async_remote_copy(
            src_ref=like, dst_ref=like, send_sem=sem, recv_sem=sem, device_id=(rows, col), device_id_type=MESH
        ).wait_recv()

    barrier = pltpu.get_barrier_semaphore()

    def greet(row, column):
        pl.semaphore_signal(barrier, inc=1, device_id=(row, column), device_id_type=MESH)

    for a, b in PEERS:
        greet(row_of(a, b), col)
        greet(row_of(a, b), before)
    greet(rows, before)
    for d in RING:
        greet(ring_row(d), col)

    own_place = pl.ds(pl.multiple_of(me * chunk, chunk), chunk)
    loads = ([], [])
    for half in range(2):
        for a, b in PEERS:
            slot = 2 * member(a, b) + half
            loads[half].append(pltpu.make_async_copy(x_hbm.at[:, slot, :], x_own.at[slot], load_sem.at[half]))
        gathered = (tops, bottoms)[half]
        loads[half].append(pltpu.make_async_copy(x_hbm.at[:, 2 * me + half, :], gathered.at[own_place], load_sem.at[half]))
        for load in loads[half]:
            load.start()
    plan_copy = pltpu.make_async_copy(plan_hbm, plan_ref, load_sem.at[2])
    plan_copy.start()

    pl.delay(1)
    pl.semaphore_wait(barrier, 2 * near + 1 + ring)

    pl.delay(1)
    for half in range(2):
        gathered = (tops, bottoms)[half]
        for load in loads[half]:
            load.wait()
        for k, (a, b) in enumerate(PEERS):
            send(
                x_own.at[2 * member(a, b) + half],
                gathered.at[own_place],
                in_send,
                in_recv.at[half, int(k >= early)],
                row_of(a, b),
                col,
            )
    plan_copy.wait()

    def ring_place(d):
        return pl.ds(pl.multiple_of(((z + d) % ZS) * share, share), share)

    pl.delay(1)
    def lines_of(gathered, batch):
        offsets = ((0, 0), *PEERS[:early]) if batch == 0 else PEERS[early:]
        places = [pl.ds(pl.multiple_of(member(XS - a, YS - b) * chunk, chunk), chunk) for a, b in offsets]
        return jnp.concatenate([gathered[place] for place in places], axis=0)

    def arrived(gathered, half, batch):
        count = near - early if batch else early
        await_bytes(gathered.at[: count * chunk], in_recv.at[half, batch])

    arrived(tops, 0, 0)
    tops_early = lines_of(tops, 0)
    square_early = full_product(tops_early, tops_early, FIRST)
    arrived(tops, 0, 1)
    pl.delay(1)
    @pl.when(col % 2 == 0)
    def _():
        send(tops, next_tops, next_send, next_recv.at[0], rows, after)

    tops_late = lines_of(tops, 1)
    partial[0] = square_early + full_product(tops_late, tops_late, FIRST)
    for n, d in enumerate(RING):
        send(partial.at[0, ring_place(d)], shares_tt.at[n], sum_send, sum_recv.at[0], ring_row(d), col)

    pl.delay(1)
    arrived(bottoms, 1, 0)
    bottoms_early = lines_of(bottoms, 0)
    both_early = full_product(bottoms_early, jnp.concatenate([tops_early, bottoms_early], axis=1), FIRST)
    arrived(bottoms, 1, 1)
    pl.delay(1)
    @pl.when(col % 2 == 1)
    def _():
        send(tops, next_tops, next_send, next_recv.at[0], rows, after)

    send(bottoms, next_bottoms, next_send, next_recv.at[1], rows, after)
    pl.delay(1)
    bottoms_late = lines_of(bottoms, 1)
    both = both_early + full_product(bottoms_late, jnp.concatenate([tops_late, bottoms_late], axis=1), FIRST)
    partial[1] = both[:, :BLOCK]
    partial[2] = both[:, BLOCK:]
    for n, d in enumerate(RING):
        send(partial.at[1:3, ring_place(d)], shares_b.at[n], sum_send, sum_recv.at[1], ring_row(d), col)

    def cross_products(half):
        arrived_block = (next_tops, next_bottoms)[half]
        await_bytes(arrived_block, next_recv.at[half])
        columns = parts_of(jnp.concatenate([tops[...], bottoms[...]], axis=1))
        between[half] = product_of(parts_of(arrived_block[...]), columns, FIRST)
        for n, d in enumerate(RING):
            send(between.at[half, ring_place(d)], shares_c.at[half, n], cross_send, cross_recv.at[half], ring_row(d), col)

    pl.delay(1)
    cross_products(0)

    pl.delay(1)
    here = ring_place(0)
    await_bytes(shares_tt, sum_recv.at[0])
    own_tt = partial[0, here]
    for n in range(ring):
        own_tt = own_tt + shares_tt[n]
    await_bytes(shares_b, sum_recv.at[1])
    own_b = partial[1:3, here]
    for n in range(ring):
        own_b = own_b + shares_b[n]
    line = lax.broadcasted_iota(jnp.int32, (share, BLOCK), 0) + z * share
    lane = lax.broadcasted_iota(jnp.int32, (share, BLOCK), 1)
    mine = jnp.stack([own_b[0], jnp.where(lane >= line, own_tt, own_b[1])], axis=0)
    total_mine[...] = mine
    total[:, here] = mine
    diagonal = jnp.sum(jnp.where(lane == line, own_b[1], 0.0), axis=0, keepdims=True)
    diagonal_mine[...] = diagonal
    diagonals[z] = diagonal
    for d in RING:
        send(total_mine, total.at[:, here], all_send, all_recv.at[0], ring_row(d), col)
        send(diagonal_mine, diagonals.at[z], all_send, all_recv.at[1], ring_row(d), col)
    pl.delay(1)
    cross_products(1)
    pl.delay(1)
    await_bytes(total.at[:, : ring * share], all_recv.at[0])
    await_bytes(diagonals.at[:ring], all_recv.at[1])

    pl.delay(1)
    cross = total[0]
    packed = total[1]
    flipped = jnp.transpose(packed)
    line = lax.broadcasted_iota(jnp.int32, (BLOCK, BLOCK), 0)
    lane = lax.broadcasted_iota(jnp.int32, (BLOCK, BLOCK), 1)
    diagonal = jnp.sum(diagonals[...], axis=0)
    top_gram = jnp.where(lane >= line, packed, flipped)
    bottom_gram = jnp.where(lane == line, diagonal, jnp.where(lane < line, packed, flipped))
    gram = jnp.concatenate(
        [
            jnp.concatenate([top_gram, jnp.transpose(cross)], axis=1),
            jnp.concatenate([cross, bottom_gram], axis=1),
        ],
        axis=0,
    )
    rounds = plan_ref.shape[1]

    def first_plan(r):
        return plan_ref[0, r : r + 1, :]

    def tell(r, cosine, sine):
        turns_out[r] = jnp.concatenate([cosine, sine], axis=0)
        send(turns_out.at[r], turns_in.at[r], next_send, next_recv.at[2 + r], rows, after)

    rotation, image = solve(gram, first_plan, rounds, tell)
    pl.delay(1)
    await_bytes(shares_c.at[0], cross_recv.at[0])
    await_bytes(shares_c.at[1], cross_recv.at[1])
    pl.delay(1)
    mine = between[:, here]
    for n in range(ring):
        mine = mine + shares_c[:, n]
    turn = parts_of(rotation)
    left = [part[:, :BLOCK] for part in turn]
    mine = product_of(parts_of(mine.reshape(2 * share, WIDTH)), left).reshape(2, share, BLOCK)
    half_turned_mine[...] = mine
    half_turned[:, here] = mine
    for d in RING:
        send(half_turned_mine, half_turned.at[:, here], all2_send, all2_recv, ring_row(d), col)
    pl.delay(1)
    square_out[...] = full_product(rotation[:, BLOCK:], image[:, BLOCK:], FIRST)
    top_square = full_product(rotation[:, :BLOCK], image[:, :BLOCK], FIRST)
    send(square_out, square_in, next_send, next_recv.at[2 + rounds], rows, after)

    pl.delay(1)
    below = lax.broadcasted_iota(jnp.int32, (WIDTH, WIDTH), 0)
    along = lax.broadcasted_iota(jnp.int32, (WIDTH, WIDTH), 1)
    columns = parts_of(jnp.concatenate([tops[...], bottoms[...]], axis=1))
    tops_now[...] = product_of(columns, left)
    next_rotation = None
    for r in range(rounds):
        moved = times_onehot(next_rotation, first_plan(r)) if r else None
        await_bytes(turns_in.at[r], next_recv.at[2 + r])
        cosine, sine = turns_in[r, 0:1, :], turns_in[r, 1:2, :]
        if r:
            next_rotation = next_rotation * cosine + moved * sine
        else:
            next_rotation = jnp.where(below == along, cosine, 0.0) + jnp.where(below == first_plan(r), sine, 0.0)
    right = [part[:, BLOCK:] for part in parts_of(next_rotation)]
    pl.delay(1)
    await_bytes(square_in, next_recv.at[2 + rounds])
    await_bytes(half_turned.at[:, : ring * share], all2_recv)
    pl.delay(1)
    cross = product_of(parts_of(half_turned[...].reshape(WIDTH, BLOCK)), right, FIRST)
    gram = jnp.concatenate(
        [jnp.concatenate([top_square, cross], axis=1), jnp.concatenate([jnp.transpose(cross), square_in[...]], axis=1)],
        axis=0,
    )
    next_columns = parts_of(jnp.concatenate([next_tops[...], next_bottoms[...]], axis=1))
    bottoms_in[...] = product_of(next_columns, right)
    rotation, _ = solve(gram, lambda r: plan_ref[1, r : r + 1, :], rounds, lambda *_: None)

    pl.delay(1)
    turn = parts_of(rotation)
    targets = PEERS + ((0, 0),)
    for first, last in ((0, 1), (1, 4), (4, 8)):
        places = [pl.ds(pl.multiple_of(member(a, b) * chunk, chunk), chunk) for a, b in targets[first:last]]
        lines = [jnp.concatenate([tops_now[place], bottoms_in[place]], axis=1) for place in places]
        now = product_of(parts_of(jnp.concatenate(lines, axis=0)), turn)
        for k in range(first, last):
            part = now[(k - first) * chunk : (k - first + 1) * chunk]
            result_out[k, 1] = part[:, BLOCK:]
            if k < near:
                result_out[k, 0] = part[:, :BLOCK]
            else:
                result[2 * me] = part[:, :BLOCK]
        for k in range(first, last):
            row = row_of(*targets[k])
            send(result_out.at[k, 1], result.at[2 * me + 1], out_send, out_recv, row, after)
            if k < near:
                send(result_out.at[k, 0], result.at[2 * me], out_send, out_recv, row, col)
    pl.delay(1)
    await_bytes(result.at[: 2 * near + 1], out_recv)
    pl.delay(1)
    await_bytes(x_own.at[: 2 * near], in_send)
    await_bytes(tops.at[: 3 * ring * share], sum_send)
    await_bytes(tops.at[: 2 * ring * share], all_send)
    await_bytes(diagonals.at[:ring], all_send)
    await_bytes(tops, next_send)
    await_bytes(bottoms, next_send)
    await_bytes(turns_out, next_send)
    await_bytes(square_out, next_send)
    await_bytes(shares_c, cross_send)
    await_bytes(half_turned.at[:, : ring * share], all2_send)
    await_bytes(result.at[: 2 * near + 1], out_send)


def place_kernel(result, out, sem):
    copies = [pltpu.make_async_copy(result.at[n], out.at[:, n, :], sem) for n in range(result.shape[0])]
    for copy in copies:
        copy.start()
    for copy in copies:
        copy.wait()


def body(matrix, plan):
    chunk, pairs, halves, width = matrix.shape
    slots = pairs * halves
    every = chunk * GROUP
    share = BLOCK // ZS
    f32 = jnp.float32
    dma = pltpu.SemaphoreType.DMA
    near, ring = len(PEERS), len(RING)
    vmem = pltpu.VMEM
    result = pl.pallas_call(
        kernel,
        out_shape=jax.ShapeDtypeStruct((slots, chunk, width), f32),
        in_specs=[pl.BlockSpec(memory_space=pltpu.HBM)] * 2,
        out_specs=pl.BlockSpec(memory_space=pltpu.VMEM),
        scratch_shapes=[
            vmem(plan.shape, jnp.int32),
            vmem((slots, chunk, width), f32),
            vmem((every, width), f32),
            vmem((every, width), f32),
            vmem((3, BLOCK, BLOCK), f32),
            vmem((ring, share, BLOCK), f32),
            vmem((ring, 2, share, BLOCK), f32),
            vmem((2, BLOCK, BLOCK), f32),
            vmem((2, share, BLOCK), f32),
            vmem((ZS, 1, BLOCK), f32),
            vmem((1, BLOCK), f32),
            vmem((every, width), f32),
            vmem((every, width), f32),
            vmem((plan.shape[1], 2, WIDTH), f32),
            vmem((plan.shape[1], 2, WIDTH), f32),
            vmem((every, width), f32),
            vmem((BLOCK, BLOCK), f32),
            vmem((BLOCK, BLOCK), f32),
            vmem((every, width), f32),
            vmem((2, BLOCK, WIDTH), f32),
            vmem((2, ring, share, WIDTH), f32),
            vmem((2, BLOCK, BLOCK), f32),
            vmem((2, share, BLOCK), f32),
            vmem((near + 1, 2, chunk, width), f32),
            dma((3,)),
            dma,
            dma((2, 2)),
            dma,
            dma((2,)),
            dma,
            dma((2,)),
            dma,
            dma((7,)),
            dma,
            dma((2,)),
            dma,
            dma,
            dma,
            dma,
        ],
        compiler_params=pltpu.CompilerParams(collective_id=0, has_side_effects=True, vmem_limit_bytes=24 * 2**20),
        cost_estimate=pl.CostEstimate(flops=10**9, bytes_accessed=2 * matrix.size * 4, transcendentals=0),
        name="jacobi_steps",
    )(pltpu.with_memory_space_constraint(matrix.reshape(chunk, slots, width), pltpu.HBM), pltpu.with_memory_space_constraint(plan, pltpu.HBM))
    placed = pl.pallas_call(
        place_kernel,
        out_shape=jax.ShapeDtypeStruct((chunk, slots, width), f32),
        in_specs=[pl.BlockSpec(memory_space=pltpu.VMEM)],
        out_specs=pl.BlockSpec(memory_space=pltpu.HBM),
        scratch_shapes=[dma],
        compiler_params=pltpu.CompilerParams(vmem_limit_bytes=2**20),
        name="place",
    )(result)
    return placed.reshape(matrix.shape)


def solution(mesh):
    in_specs = (P("rows", "cols", None, None), P())
    out_specs = P("rows", "cols", None, None)
    return jax.shard_map(body, mesh=mesh, in_specs=in_specs, out_specs=out_specs, check_vma=False)
```

```python
import functools

import jax
import jax.numpy as jnp
from jax import lax
from jax.experimental import pallas as pl
from jax.experimental.pallas import tpu as pltpu
from jax.sharding import PartitionSpec as P

MESH = pl.DeviceIdType.MESH
XS, ZS, YS, CS = 4, 8, 2, 4
GROUP = XS * YS
BLOCK = 128
WIDTH = 2 * BLOCK
PEERS = ((2, 1), (0, 1), (1, 1), (2, 0), (3, 1), (1, 0), (3, 0))
RING = (4, 3, 5, 2, 6, 1, 7)
FIRST = (((0,), (0,)), ((), ()))
PLAIN = (((1,), (0,)), ((), ()))


def parts_of(value):
    high = value.astype(jnp.bfloat16)
    rest = value - high.astype(jnp.float32)
    middle = rest.astype(jnp.bfloat16)
    low = (rest - middle.astype(jnp.float32)).astype(jnp.bfloat16)
    return high, middle, low


def product(a, b, dims):
    return lax.dot_general(a, b, dims, preferred_element_type=jnp.float32)


def full_product(a, b, dims=PLAIN):
    return lax.dot_general(
        a, b, dims, precision=lax.Precision.HIGHEST, preferred_element_type=jnp.float32
    )


def product_of(a, b, dims=PLAIN):
    high = product(a[0], b[0], dims)
    return high + (product(a[0], b[1], dims) + product(a[1], b[0], dims))


def times_onehot(value, partner):
    rows = lax.broadcasted_iota(jnp.int32, (WIDTH, WIDTH), 0)
    onehot = (rows == partner).astype(jnp.float32).astype(jnp.bfloat16)
    high, middle, low = parts_of(value)
    return product(high, onehot, PLAIN) + (product(middle, onehot, PLAIN) + product(low, onehot, PLAIN))


def columns_moved(value, partner):
    rows = value.shape[0]
    near = jnp.where(partner < BLOCK, partner, partner - BLOCK)
    sides = []
    for half in range(2):
        lanes = slice(half * BLOCK, (half + 1) * BLOCK)
        index = jnp.broadcast_to(near[:, lanes], (rows, BLOCK))
        left = jnp.broadcast_to(partner[:, lanes] < BLOCK, (rows, BLOCK))
        picked = [
            jnp.take_along_axis(value[:, n * BLOCK : (n + 1) * BLOCK], index, axis=1, mode="promise_in_bounds")
            for n in range(2)
        ]
        sides.append(jnp.where(left, picked[0], picked[1]))
    return jnp.concatenate(sides, axis=1)


def solve(gram, plan_of_round, rounds, tell):
    below = lax.broadcasted_iota(jnp.int32, (WIDTH, WIDTH), 0)
    along = lax.broadcasted_iota(jnp.int32, (WIDTH, WIDTH), 1)
    index = lax.broadcasted_iota(jnp.int32, (1, WIDTH), 1)
    rotation = None
    image = gram
    for r in range(rounds):
        partner = plan_of_round(r)
        if r == 0:
            unit = below == along
            pairing = below == partner
            own = jnp.sum(jnp.where(unit, gram, 0.0), axis=0, keepdims=True)
            cross = jnp.sum(jnp.where(pairing, gram, 0.0), axis=0, keepdims=True)
        else:
            own = jnp.sum(rotation * image, axis=0, keepdims=True)
            rotation_moved = columns_moved(rotation, partner)
            cross = jnp.sum(rotation_moved * image, axis=0, keepdims=True)
        other = columns_moved(jnp.broadcast_to(own, (8, WIDTH)), partner)[:1]
        orient = jnp.where(index < partner, 1.0, -1.0)
        spread = orient * (other - own)
        sign = jnp.where(spread >= 0.0, 1.0, -1.0)
        tangent = sign * 2.0 * cross / (jnp.abs(spread) + jnp.sqrt(spread * spread + 4.0 * cross * cross))
        cosine = lax.rsqrt(1.0 + tangent * tangent)
        sine = -orient * (tangent * cosine)
        tell(r, cosine, sine)
        if r == 0:
            rotation = jnp.where(unit, cosine, 0.0) + jnp.where(pairing, sine, 0.0)
        else:
            rotation = rotation * cosine + rotation_moved * sine
        image = image * cosine + columns_moved(image, partner) * sine
    return rotation, image


def kernel(
    x_hbm,
    plan_hbm,
    result,
    plan_ref,
    x_own,
    tops,
    bottoms,
    partial,
    shares_tt,
    shares_b,
    total,
    total_mine,
    diagonals,
    diagonal_mine,
    next_tops,
    next_bottoms,
    turns_out,
    turns_in,
    bottoms_in,
    square_out,
    square_in,
    tops_now,
    between,
    shares_c,
    half_turned,
    half_turned_mine,
    result_out,
    load_sem,
    in_send,
    in_recv,
    sum_send,
    sum_recv,
    all_send,
    all_recv,
    next_send,
    next_recv,
    cross_send,
    cross_recv,
    all2_send,
    all2_recv,
    out_send,
    out_recv,
):
    rows = lax.axis_index("rows")
    col = lax.axis_index("cols")
    x = rows // (ZS * YS)
    z = (rows // YS) % ZS
    y = rows % YS
    me = x * YS + y
    chunk = x_own.shape[1]
    every = tops.shape[0]
    share = BLOCK // ZS
    near, ring = len(PEERS), len(RING)
    early = near // 2

    def member(a, b):
        return ((x + a) % XS) * YS + (y + b) % YS

    def row_of(a, b):
        return (((x + a) % XS) * ZS + z) * YS + (y + b) % YS

    def ring_row(d):
        return (x * ZS + (z + d) % ZS) * YS + y

    after = (col + 1) % CS
    before = (col + CS - 1) % CS

    def send(src, dst, send_sem, recv_sem, row, column):
        pltpu.make_async_remote_copy(
            src_ref=src, dst_ref=dst, send_sem=send_sem, recv_sem=recv_sem, device_id=(row, column), device_id_type=MESH
        ).start()

    def await_bytes(like, sem):
        pltpu.make_async_remote_copy(
            src_ref=like, dst_ref=like, send_sem=sem, recv_sem=sem, device_id=(rows, col), device_id_type=MESH
        ).wait_recv()

    barrier = pltpu.get_barrier_semaphore()

    def greet(row, column):
        pl.semaphore_signal(barrier, inc=1, device_id=(row, column), device_id_type=MESH)

    for a, b in PEERS:
        greet(row_of(a, b), col)
        greet(row_of(a, b), before)
    greet(rows, before)
    for d in RING:
        greet(ring_row(d), col)

    own_place = pl.ds(pl.multiple_of(me * chunk, chunk), chunk)
    loads = ([], [])
    for half in range(2):
        for a, b in PEERS:
            slot = 2 * member(a, b) + half
            loads[half].append(pltpu.make_async_copy(x_hbm.at[:, slot, :], x_own.at[slot], load_sem.at[half]))
        gathered = (tops, bottoms)[half]
        loads[half].append(pltpu.make_async_copy(x_hbm.at[:, 2 * me + half, :], gathered.at[own_place], load_sem.at[half]))
        for load in loads[half]:
            load.start()
    plan_copy = pltpu.make_async_copy(plan_hbm, plan_ref, load_sem.at[2])
    plan_copy.start()

    pl.delay(1)
    pl.semaphore_wait(barrier, 2 * near + 1 + ring)

    pl.delay(1)
    for half in range(2):
        gathered = (tops, bottoms)[half]
        for load in loads[half]:
            load.wait()
        for k, (a, b) in enumerate(PEERS):
            send(
                x_own.at[2 * member(a, b) + half],
                gathered.at[own_place],
                in_send,
                in_recv.at[half, int(k >= early)],
                row_of(a, b),
                col,
            )
    plan_copy.wait()

    def ring_place(d):
        return pl.ds(pl.multiple_of(((z + d) % ZS) * share, share), share)

    pl.delay(1)
    def lines_of(gathered, batch):
        offsets = ((0, 0), *PEERS[:early]) if batch == 0 else PEERS[early:]
        places = [pl.ds(pl.multiple_of(member(XS - a, YS - b) * chunk, chunk), chunk) for a, b in offsets]
        return jnp.concatenate([gathered[place] for place in places], axis=0)

    def arrived(gathered, half, batch):
        count = near - early if batch else early
        await_bytes(gathered.at[: count * chunk], in_recv.at[half, batch])

    arrived(tops, 0, 0)
    tops_early = lines_of(tops, 0)
    square_early = full_product(tops_early, tops_early, FIRST)
    arrived(tops, 0, 1)
    pl.delay(1)
    @pl.when(col % 2 == 0)
    def _():
        send(tops, next_tops, next_send, next_recv.at[0], rows, after)

    tops_late = lines_of(tops, 1)
    partial[0] = square_early + full_product(tops_late, tops_late, FIRST)
    for n, d in enumerate(RING):
        send(partial.at[0, ring_place(d)], shares_tt.at[n], sum_send, sum_recv.at[0], ring_row(d), col)

    pl.delay(1)
    arrived(bottoms, 1, 0)
    bottoms_early = lines_of(bottoms, 0)
    both_early = full_product(bottoms_early, jnp.concatenate([tops_early, bottoms_early], axis=1), FIRST)
    arrived(bottoms, 1, 1)
    pl.delay(1)
    @pl.when(col % 2 == 1)
    def _():
        send(tops, next_tops, next_send, next_recv.at[0], rows, after)

    send(bottoms, next_bottoms, next_send, next_recv.at[1], rows, after)
    pl.delay(1)
    bottoms_late = lines_of(bottoms, 1)
    both = both_early + full_product(bottoms_late, jnp.concatenate([tops_late, bottoms_late], axis=1), FIRST)
    partial[1] = both[:, :BLOCK]
    partial[2] = both[:, BLOCK:]
    for n, d in enumerate(RING):
        send(partial.at[1:3, ring_place(d)], shares_b.at[n], sum_send, sum_recv.at[1], ring_row(d), col)

    def cross_products(half):
        arrived_block = (next_tops, next_bottoms)[half]
        await_bytes(arrived_block, next_recv.at[half])
        columns = parts_of(jnp.concatenate([tops[...], bottoms[...]], axis=1))
        between[half] = product_of(parts_of(arrived_block[...]), columns, FIRST)
        for n, d in enumerate(RING):
            send(between.at[half, ring_place(d)], shares_c.at[half, n], cross_send, cross_recv.at[half], ring_row(d), col)

    pl.delay(1)
    cross_products(0)

    pl.delay(1)
    here = ring_place(0)
    await_bytes(shares_tt, sum_recv.at[0])
    own_tt = partial[0, here]
    for n in range(ring):
        own_tt = own_tt + shares_tt[n]
    await_bytes(shares_b, sum_recv.at[1])
    own_b = partial[1:3, here]
    for n in range(ring):
        own_b = own_b + shares_b[n]
    line = lax.broadcasted_iota(jnp.int32, (share, BLOCK), 0) + z * share
    lane = lax.broadcasted_iota(jnp.int32, (share, BLOCK), 1)
    mine = jnp.stack([own_b[0], jnp.where(lane >= line, own_tt, own_b[1])], axis=0)
    total_mine[...] = mine
    total[:, here] = mine
    diagonal = jnp.sum(jnp.where(lane == line, own_b[1], 0.0), axis=0, keepdims=True)
    diagonal_mine[...] = diagonal
    diagonals[z] = diagonal
    for d in RING:
        send(total_mine, total.at[:, here], all_send, all_recv.at[0], ring_row(d), col)
        send(diagonal_mine, diagonals.at[z], all_send, all_recv.at[1], ring_row(d), col)
    pl.delay(1)
    cross_products(1)
    pl.delay(1)
    await_bytes(total.at[:, : ring * share], all_recv.at[0])
    await_bytes(diagonals.at[:ring], all_recv.at[1])

    pl.delay(1)
    cross = total[0]
    packed = total[1]
    flipped = jnp.transpose(packed)
    line = lax.broadcasted_iota(jnp.int32, (BLOCK, BLOCK), 0)
    lane = lax.broadcasted_iota(jnp.int32, (BLOCK, BLOCK), 1)
    diagonal = jnp.sum(diagonals[...], axis=0)
    top_gram = jnp.where(lane >= line, packed, flipped)
    bottom_gram = jnp.where(lane == line, diagonal, jnp.where(lane < line, packed, flipped))
    gram = jnp.concatenate(
        [
            jnp.concatenate([top_gram, jnp.transpose(cross)], axis=1),
            jnp.concatenate([cross, bottom_gram], axis=1),
        ],
        axis=0,
    )
    rounds = plan_ref.shape[1]

    def first_plan(r):
        return plan_ref[0, r : r + 1, :]

    def tell(r, cosine, sine):
        turns_out[r] = jnp.concatenate([cosine, sine], axis=0)

    rotation, image = solve(gram, first_plan, rounds, tell)
    send(turns_out, turns_in, next_send, next_recv.at[2], rows, after)
    pl.delay(1)
    await_bytes(shares_c.at[0], cross_recv.at[0])
    await_bytes(shares_c.at[1], cross_recv.at[1])
    pl.delay(1)
    mine = between[:, here]
    for n in range(ring):
        mine = mine + shares_c[:, n]
    turn = parts_of(rotation)
    left = [part[:, :BLOCK] for part in turn]
    mine = product_of(parts_of(mine.reshape(2 * share, WIDTH)), left).reshape(2, share, BLOCK)
    half_turned_mine[...] = mine
    half_turned[:, here] = mine
    for d in RING:
        send(half_turned_mine, half_turned.at[:, here], all2_send, all2_recv, ring_row(d), col)
    pl.delay(1)
    square_out[...] = full_product(rotation[:, BLOCK:], image[:, BLOCK:], FIRST)
    top_square = full_product(rotation[:, :BLOCK], image[:, :BLOCK], FIRST)
    send(square_out, square_in, next_send, next_recv.at[2 + rounds], rows, after)

    pl.delay(1)
    below = lax.broadcasted_iota(jnp.int32, (WIDTH, WIDTH), 0)
    along = lax.broadcasted_iota(jnp.int32, (WIDTH, WIDTH), 1)
    columns = parts_of(jnp.concatenate([tops[...], bottoms[...]], axis=1))
    tops_now[...] = product_of(columns, left)
    next_rotation = None
    for r in range(rounds):
        moved = times_onehot(next_rotation, first_plan(r)) if r else None
        if r == 0:
            await_bytes(turns_in, next_recv.at[2])
        cosine, sine = turns_in[r, 0:1, :], turns_in[r, 1:2, :]
        if r:
            next_rotation = next_rotation * cosine + moved * sine
        else:
            next_rotation = jnp.where(below == along, cosine, 0.0) + jnp.where(below == first_plan(r), sine, 0.0)
    right = [part[:, BLOCK:] for part in parts_of(next_rotation)]
    pl.delay(1)
    await_bytes(square_in, next_recv.at[2 + rounds])
    await_bytes(half_turned.at[:, : ring * share], all2_recv)
    pl.delay(1)
    cross = product_of(parts_of(half_turned[...].reshape(WIDTH, BLOCK)), right, FIRST)
    gram = jnp.concatenate(
        [jnp.concatenate([top_square, cross], axis=1), jnp.concatenate([jnp.transpose(cross), square_in[...]], axis=1)],
        axis=0,
    )
    next_columns = parts_of(jnp.concatenate([next_tops[...], next_bottoms[...]], axis=1))
    bottoms_in[...] = product_of(next_columns, right)
    rotation, _ = solve(gram, lambda r: plan_ref[1, r : r + 1, :], rounds, lambda *_: None)

    pl.delay(1)
    turn = parts_of(rotation)
    targets = PEERS + ((0, 0),)
    for first, last in ((0, 1), (1, 4), (4, 8)):
        places = [pl.ds(pl.multiple_of(member(a, b) * chunk, chunk), chunk) for a, b in targets[first:last]]
        lines = [jnp.concatenate([tops_now[place], bottoms_in[place]], axis=1) for place in places]
        now = product_of(parts_of(jnp.concatenate(lines, axis=0)), turn)
        for k in range(first, last):
            part = now[(k - first) * chunk : (k - first + 1) * chunk]
            result_out[k, 1] = part[:, BLOCK:]
            if k < near:
                result_out[k, 0] = part[:, :BLOCK]
            else:
                result[2 * me] = part[:, :BLOCK]
        for k in range(first, last):
            row = row_of(*targets[k])
            send(result_out.at[k, 1], result.at[2 * me + 1], out_send, out_recv, row, after)
            if k < near:
                send(result_out.at[k, 0], result.at[2 * me], out_send, out_recv, row, col)
    pl.delay(1)
    await_bytes(result.at[: 2 * near + 1], out_recv)
    pl.delay(1)
    await_bytes(x_own.at[: 2 * near], in_send)
    await_bytes(tops.at[: 3 * ring * share], sum_send)
    await_bytes(tops.at[: 2 * ring * share], all_send)
    await_bytes(diagonals.at[:ring], all_send)
    await_bytes(tops, next_send)
    await_bytes(bottoms, next_send)
    await_bytes(turns_out, next_send)
    await_bytes(square_out, next_send)
    await_bytes(shares_c, cross_send)
    await_bytes(half_turned.at[:, : ring * share], all2_send)
    await_bytes(result.at[: 2 * near + 1], out_send)


def place_kernel(result, out, sem):
    copies = [pltpu.make_async_copy(result.at[n], out.at[:, n, :], sem) for n in range(result.shape[0])]
    for copy in copies:
        copy.start()
    for copy in copies:
        copy.wait()


def body(matrix, plan):
    chunk, pairs, halves, width = matrix.shape
    slots = pairs * halves
    every = chunk * GROUP
    share = BLOCK // ZS
    f32 = jnp.float32
    dma = pltpu.SemaphoreType.DMA
    near, ring = len(PEERS), len(RING)
    vmem = pltpu.VMEM
    result = pl.pallas_call(
        kernel,
        out_shape=jax.ShapeDtypeStruct((slots, chunk, width), f32),
        in_specs=[pl.BlockSpec(memory_space=pltpu.HBM)] * 2,
        out_specs=pl.BlockSpec(memory_space=pltpu.VMEM),
        scratch_shapes=[
            vmem(plan.shape, jnp.int32),
            vmem((slots, chunk, width), f32),
            vmem((every, width), f32),
            vmem((every, width), f32),
            vmem((3, BLOCK, BLOCK), f32),
            vmem((ring, share, BLOCK), f32),
            vmem((ring, 2, share, BLOCK), f32),
            vmem((2, BLOCK, BLOCK), f32),
            vmem((2, share, BLOCK), f32),
            vmem((ZS, 1, BLOCK), f32),
            vmem((1, BLOCK), f32),
            vmem((every, width), f32),
            vmem((every, width), f32),
            vmem((plan.shape[1], 2, WIDTH), f32),
            vmem((plan.shape[1], 2, WIDTH), f32),
            vmem((every, width), f32),
            vmem((BLOCK, BLOCK), f32),
            vmem((BLOCK, BLOCK), f32),
            vmem((every, width), f32),
            vmem((2, BLOCK, WIDTH), f32),
            vmem((2, ring, share, WIDTH), f32),
            vmem((2, BLOCK, BLOCK), f32),
            vmem((2, share, BLOCK), f32),
            vmem((near + 1, 2, chunk, width), f32),
            dma((3,)),
            dma,
            dma((2, 2)),
            dma,
            dma((2,)),
            dma,
            dma((2,)),
            dma,
            dma((7,)),
            dma,
            dma((2,)),
            dma,
            dma,
            dma,
            dma,
        ],
        compiler_params=pltpu.CompilerParams(collective_id=0, has_side_effects=True, vmem_limit_bytes=24 * 2**20),
        cost_estimate=pl.CostEstimate(flops=10**9, bytes_accessed=2 * matrix.size * 4, transcendentals=0),
        name="jacobi_steps",
    )(pltpu.with_memory_space_constraint(matrix.reshape(chunk, slots, width), pltpu.HBM), pltpu.with_memory_space_constraint(plan, pltpu.HBM))
    placed = pl.pallas_call(
        place_kernel,
        out_shape=jax.ShapeDtypeStruct((chunk, slots, width), f32),
        in_specs=[pl.BlockSpec(memory_space=pltpu.VMEM)],
        out_specs=pl.BlockSpec(memory_space=pltpu.HBM),
        scratch_shapes=[dma],
        compiler_params=pltpu.CompilerParams(vmem_limit_bytes=2**20),
        name="place",
    )(result)
    return placed.reshape(matrix.shape)


def solution(mesh):
    in_specs = (P("rows", "cols", None, None), P())
    out_specs = P("rows", "cols", None, None)
    return jax.shard_map(body, mesh=mesh, in_specs=in_specs, out_specs=out_specs, check_vma=False)
```
